32 devices in a mesh: rep: 2 (over x), dp: 16 (over y, z, core).
Axes of the slice: x: 2, y: 2, z: 4, core: 2. Of those that a mesh axis runs over, the one named last changes fastest.
Arguments:
- g_w_gate: bfloat16 [32, 2, 1024, 4096], P(('rep', 'dp')), parts along dimension 0
- g_w_up: bfloat16 [32, 2, 1024, 4096], P(('rep', 'dp')), parts along dimension 0
- g_w_down: bfloat16 [32, 2, 4096, 1024], P(('rep', 'dp')), parts along dimension 0
- w_gate: bfloat16 [2, 1024, 4096], replicated
- w_up: bfloat16 [2, 1024, 4096], replicated
- w_down: bfloat16 [2, 4096, 1024], replicated
- m_w_gate: float32 [2, 1024, 4096], P(None, 'dp')
- m_w_up: float32 [2, 1024, 4096], P(None, 'dp')
- m_w_down: float32 [2, 4096, 1024], P(None, 'dp')
- v_w_gate: float32 [2, 1024, 4096], P(None, 'dp')
- v_w_up: float32 [2, 1024, 4096], P(None, 'dp')
- v_w_down: float32 [2, 4096, 1024], P(None, 'dp')
Outputs:
- output 1: bfloat16 [4, 1024, 4096], P('rep'), parts along dimension 0
- output 2: bfloat16 [4, 1024, 4096], P('rep'), parts along dimension 0
- output 3: bfloat16 [4, 4096, 1024], P('rep'), parts along dimension 0
- output 4: float32 [4, 1024, 4096], P('rep', 'dp'), parts along dimension 0
- output 5: float32 [4, 1024, 4096], P('rep', 'dp'), parts along dimension 0
- output 6: float32 [4, 4096, 1024], P('rep', 'dp'), parts along dimension 0
- output 7: float32 [4, 1024, 4096], P('rep', 'dp'), parts along dimension 0
- output 8: float32 [4, 1024, 4096], P('rep', 'dp'), parts along dimension 0
- output 9: float32 [4, 4096, 1024], P('rep', 'dp'), parts along dimension 0
There are 2 independent parts. The reference program is written for one: setup_inputs(seed, part) draws one part's arguments, and reference() takes and returns one part's arrays. A program takes and returns all parts, laid end to end along the dimension named above; an argument that names none is the same for every part.
All inputs are finite; a program needn't handle non-finite values.
Results may differ from the reference program's by a relative error of at most 0.022.
Values are sent between devices in bfloat16 or wider.
A program may use at most 2 GiB of HBM per device.

```python
import jax
import jax.numpy as jnp
from jax import lax

DEVICES = 16
D = 1024
FF = 4096
LAYERS = 2
NAMES = ("w_gate", "w_up", "w_down")
SHAPES = {"w_gate": (LAYERS, D, FF), "w_up": (LAYERS, D, FF), "w_down": (LAYERS, FF, D)}


def setup_inputs(seed: int = 0, part: int = 0) -> dict:
    kz, *keys = jax.random.split(jax.random.key(seed), 1 + 5 * len(NAMES))
    loud = 2.0 ** jax.random.uniform(kz, (), jnp.float32, -1.0, 1.0)
    drawn = {}
    for name, key, both in zip(NAMES, keys[:3], keys[3:6], strict=True):
        own = jax.random.normal(jax.random.fold_in(key, part), (DEVICES, *SHAPES[name]), jnp.float32)
        shared = jax.random.normal(jax.random.fold_in(both, part), SHAPES[name], jnp.float32)
        drawn["g_" + name] = (loud * (0.7 * shared / DEVICES + 0.7 * own * DEVICES**-0.5)).astype(jnp.bfloat16)
    for name, key in zip(NAMES, keys[6:9], strict=True):
        drawn[name] = (jax.random.normal(key, SHAPES[name], jnp.float32) * SHAPES[name][1] ** -0.5).astype(jnp.bfloat16)
    for name, key in zip(NAMES, keys[9:12], strict=True):
        drawn["m_" + name] = loud * 0.5 * jax.random.normal(key, SHAPES[name], jnp.float32)
    for name, key in zip(NAMES, keys[12:15], strict=True):
        drawn["v_" + name] = loud * loud * jax.random.uniform(key, SHAPES[name], jnp.float32, 0.5, 1.5)
    return drawn


def adamw(w, m, v, g):
    m = 0.9 * m + 0.1 * g
    v = 0.95 * v + 0.05 * g * g
    step = m * lax.rsqrt(v + 1e-8) + 0.1 * w
    return (w - 0.02 * step).astype(jnp.bfloat16), m, v


def clipped(gradients, sum_of_squares, count):
    factor = jnp.minimum(1.0, 0.5 * lax.rsqrt(sum_of_squares / count + 1e-30))
    return [g * factor for g in gradients]


def reference(g_w_gate, g_w_up, g_w_down, w_gate, w_up, w_down, m_w_gate, m_w_up, m_w_down, v_w_gate, v_w_up, v_w_down):
    def total(terms):
        return lax.scan(lambda so_far, term: (so_far + term.astype(jnp.float32), None), jnp.zeros(terms.shape[1:], jnp.float32), terms)[0]

    gradients = [total(terms).astype(jnp.bfloat16).astype(jnp.float32) for terms in (g_w_gate, g_w_up, g_w_down)]
    gradients = clipped(gradients, sum(jnp.sum(g * g) for g in gradients), sum(g.size for g in gradients))
    new = [
        adamw(w.astype(jnp.float32), m, v, g)
        for w, m, v, g in zip((w_gate, w_up, w_down), (m_w_gate, m_w_up, m_w_down), (v_w_gate, v_w_up, v_w_down), gradients, strict=True)
    ]
    return tuple(one[which] for which in range(3) for one in new)
```

```python
import jax
import jax.numpy as jnp
from jax import lax
from jax.experimental import pallas as pl
from jax.experimental.pallas import tpu as pltpu
from jax.sharding import PartitionSpec as P

MESH = pl.DeviceIdType.MESH
F32 = jnp.float32
BF16 = jnp.bfloat16
CHIPS = 8
CHUNKS = [(d, w) for w in range(3) for d in range(2)]


def device_at(q, c):
    y = q // 4
    z = q + y * (7 - 2 * q)
    return y * 8 + z * 2 + c


def tiles(ref, body):
    rows, cols = ref.shape

    def strip(r, carry):
        at = pl.ds(pl.multiple_of(r * 16, 16), 16)
        for k in range(cols // 1024):
            body(at, pl.ds(k * 1024, 1024))
        return carry

    lax.fori_loop(0, rows // 16, strip, 0)


def kernel(*refs):
    g, wt, m, v = (refs[i : i + 3] for i in (0, 3, 6, 9))
    x, gsum = refs[12:15], refs[15:18]
    factor_ref = refs[18]
    (p_gu, p_dn, r_gu, r_dn, o_gu, o_dn, w_gu, w_dn, m_gu, m_dn, v_gu, v_dn, acc, norms) = refs[19:33]
    (p_send, p_recv, r_send, r_recv, o_sem, state_sem, a_send, a_recv, n_send, n_recv, l_sem, g_sem) = refs[33:]

    rep, dp = lax.axis_index("rep"), lax.axis_index("dp")
    y, z, c = dp // 8, (dp // 2) % 4, dp % 2
    q = z + y * (7 - 2 * z)
    nxt = [(rep, device_at((q + 1) % CHIPS, c)), (rep, device_at((q + 7) % CHIPS, c))]
    partner = (rep, dp + 1 - 2 * c)

    def pick(gu, dn, lead, d, w):
        return gu.at[(*lead, d, w)] if w < 2 else dn.at[(*lead, d)]

    def rows_of(array, w, d, dev, lead=()):
        n = 64 if w < 2 else 256
        return array[w].at[(*lead, d, pl.ds(pl.multiple_of(dev * n, n), n), slice(None))]

    def scattered(s, d):
        return (q + 7 - s + CHIPS) % CHIPS if d == 0 else (q + 1 + s) % CHIPS

    def gathered(h, d):
        return (q + CHIPS - h) % CHIPS if d == 0 else (q + h) % CHIPS

    def own_load(s, d, w):
        return pltpu.make_async_copy(
            rows_of(g, w, d, device_at(scattered(s, d), c), (0,)), pick(o_gu, o_dn, (s % 2,), d, w), o_sem.at[s % 2, d * 3 + w]
        )

    def to_partner(s, d, w):
        return pltpu.make_async_remote_copy(
            rows_of(g, w, d, device_at(scattered(s, d), 1 - c), (0,)),
            pick(p_gu, p_dn, (s,), d, w),
            p_send.at[s, d * 3 + w],
            p_recv.at[s, d * 3 + w],
            device_id=partner,
            device_id_type=MESH,
        )

    def hop(s, d, w):
        return pltpu.make_async_remote_copy(
            pick(p_gu, p_dn, (s,), d, w),
            pick(r_gu, r_dn, (s % 3,), d, w),
            r_send.at[s % 3, d * 3 + w],
            r_recv.at[s % 3, d * 3 + w],
            device_id=nxt[d],
            device_id_type=MESH,
        )

    def state_loads(d, w):
        i = d * 3 + w
        return [
            pltpu.make_async_copy(m[w].at[d], pick(m_gu, m_dn, (), d, w), state_sem.at[0, i]),
            pltpu.make_async_copy(v[w].at[d], pick(v_gu, v_dn, (), d, w), state_sem.at[1, i]),
            pltpu.make_async_copy(rows_of(wt, w, d, dp), pick(w_gu, w_dn, (), d, w), state_sem.at[2, i]),
        ]

    barrier = pltpu.get_barrier_semaphore()
    for dev in (*nxt, partner):
        pl.semaphore_signal(barrier, inc=1, device_id=dev, device_id_type=MESH)
    for d, w in CHUNKS:
        own_load(0, d, w).start()
    pl.semaphore_wait(barrier, 3)
    for s in (0, 1):
        for d, w in CHUNKS:
            to_partner(s, d, w).start()

    def scatter_step(s, first, last):
        if not last:
            for d, w in CHUNKS:
                own_load(s + 1, d, w).start()
            if first:
                for d, w in CHUNKS:
                    to_partner(s + 2, d, w).start()
            else:

                @pl.when(s < 6)
                def _():
                    for d, w in CHUNKS:
                        to_partner(s + 2, d, w).start()

        for d, w in CHUNKS:
            own, theirs = pick(o_gu, o_dn, (s % 2,), d, w), pick(p_gu, p_dn, (s,), d, w)
            own_load(s, d, w).wait()
            to_partner(s, d, w).wait()
            if first:

                def add(rows, cols):
                    theirs[rows, cols] = (own[rows, cols].astype(F32) + theirs[rows, cols].astype(F32)).astype(BF16)

            else:
                before = (s + 2) % 3
                so_far = pick(r_gu, r_dn, (before,), d, w)
                hop(s - 1, d, w).wait_recv()

                def add(rows, cols):
                    total = (own[rows, cols].astype(F32) + theirs[rows, cols].astype(F32)) + so_far[rows, cols].astype(F32)
                    total = total.astype(BF16)
                    theirs[rows, cols] = total
                    if last:
                        acc[...] += total.astype(F32) * total.astype(F32)

            tiles(theirs, add)
            if last:
                pltpu.make_async_copy(theirs, gsum[w].at[d], g_sem.at[d * 3 + w]).start()
            else:
                if not first:

                    @pl.when(s >= 3)
                    def _():
                        hop(s - 3, d, w).wait_send()

                hop(s, d, w).start()

    scatter_step(0, True, False)
    for d, w in CHUNKS:
        for copy in state_loads(d, w):
            copy.start()
    acc[...] = jnp.zeros_like(acc)
    lax.fori_loop(1, 7, lambda s, carry: (scatter_step(s, False, False), carry)[1], 0)
    scatter_step(7, False, True)

    mine = acc[0:8, 0:128] + acc[8:16, 0:128]
    for k in range(1, 8):
        at = pl.ds(k * 128, 128)
        mine += acc[0:8, at] + acc[8:16, at]
    norms[dp] = mine

    def norm_to(r):
        return pltpu.make_async_remote_copy(
            norms.at[dp], norms.at[dp], n_send.at[r], n_recv.at[dp], device_id=(rep, (dp + r) % 16), device_id_type=MESH
        )

    def norm_from(r):
        src = (dp + 16 - r) % 16
        return pltpu.make_async_remote_copy(
            norms.at[src], norms.at[src], n_send.at[r], n_recv.at[src], device_id=(rep, src), device_id_type=MESH
        )

    for r in range(1, 16):
        norm_to(r).start()
    for s in (4, 5, 6):
        for d, w in CHUNKS:
            hop(s, d, w).wait_send()
    for d, w in CHUNKS:
        for copy in state_loads(d, w):
            copy.wait()
    for r in range(1, 16):
        norm_from(r).wait_recv()
    squares = norms[0]
    for k in range(1, 16):
        squares += norms[k]
    count = 16 * 2 * (64 * 4096 * 2 + 256 * 1024)
    mean = jnp.sum(squares) * (1.0 / count)
    factor = jnp.minimum(1.0, 0.5 * lax.rsqrt(jnp.full((8, 128), mean, F32) + 1e-30))
    factor_ref[...] = factor
    scale = jnp.broadcast_to(factor[0:1, 0:1], (16, 1024))

    def gather_hop(h, d, w):
        block = device_at(gathered(h, d), c)
        src = pick(p_gu, p_dn, (0,), d, w) if isinstance(h, int) and h == 0 else rows_of(x, w, d, block)
        return pltpu.make_async_remote_copy(
            src, rows_of(x, w, d, block), a_send.at[h, d * 3 + w], a_recv.at[h, d * 3 + w], device_id=nxt[d], device_id_type=MESH
        )

    def gather_from(h, d, w):
        block = rows_of(x, w, d, device_at(gathered(h, d), c))
        return pltpu.make_async_remote_copy(
            block, block, a_send.at[h - 1, d * 3 + w], a_recv.at[h - 1, d * 3 + w], device_id=nxt[d], device_id_type=MESH
        )

    def share(h, d, w):
        block = device_at(gathered(h, d), c)
        src = pick(p_gu, p_dn, (0,), d, w) if isinstance(h, int) and h == 0 else rows_of(x, w, d, block)
        return pltpu.make_async_remote_copy(
            src, rows_of(x, w, d, block), p_send.at[h, d * 3 + w], p_recv.at[h, d * 3 + w], device_id=partner, device_id_type=MESH
        )

    def shared(h, d, w):
        block = rows_of(x, w, d, device_at(gathered(h, d), 1 - c))
        return pltpu.make_async_remote_copy(
            block, block, p_send.at[h, d * 3 + w], p_recv.at[h, d * 3 + w], device_id=partner, device_id_type=MESH
        )

    def keep(d, w):
        return pltpu.make_async_copy(pick(p_gu, p_dn, (0,), d, w), rows_of(x, w, d, dp), l_sem.at[d * 3 + w])

    for d, w in CHUNKS:
        gr, new = pick(p_gu, p_dn, (7,), d, w), pick(p_gu, p_dn, (0,), d, w)
        mr, vr, wr = pick(m_gu, m_dn, (), d, w), pick(v_gu, v_dn, (), d, w), pick(w_gu, w_dn, (), d, w)

        def update(rows, cols):
            grad = gr[rows, cols].astype(F32) * scale
            m1 = 0.9 * mr[rows, cols] + 0.1 * grad
            v1 = 0.95 * vr[rows, cols] + 0.05 * grad * grad
            old = wr[rows, cols].astype(F32)
            new[rows, cols] = (old - 0.02 * (m1 * lax.rsqrt(v1 + 1e-8) + 0.1 * old)).astype(BF16)

        tiles(new, update)
        gather_hop(0, d, w).start()
        share(0, d, w).start()
        keep(d, w).start()

    def gather_step(h, carry):
        for d, w in CHUNKS:
            gather_from(h, d, w).wait_recv()
            gather_hop(h, d, w).start()
            share(h, d, w).start()
        return carry

    lax.fori_loop(1, 7, gather_step, 0)
    for d, w in CHUNKS:
        gather_from(7, d, w).wait_recv()
        share(7, d, w).start()

    for r in range(1, 16):
        norm_to(r).wait_send()
    for d, w in CHUNKS:
        keep(d, w).wait()
        pltpu.make_async_copy(pick(p_gu, p_dn, (7,), d, w), gsum[w].at[d], g_sem.at[d * 3 + w]).wait()

    def drain(h, carry):
        for d, w in CHUNKS:
            gather_from(h + 1, d, w).wait_send()
        return carry

    lax.fori_loop(0, 7, drain, 0)

    def drain_shares(h, carry):
        for d, w in CHUNKS:
            shared(h, d, w).wait()
        return carry

    lax.fori_loop(0, 8, drain_shares, 0)


def solution(mesh):
    whole = [(2, 1024, 4096), (2, 1024, 4096), (2, 4096, 1024)]
    block = [(2, 64, 4096), (2, 64, 4096), (2, 256, 1024)]

    def pair(lead, dtype):
        return [pltpu.VMEM((*lead, 2, 2, 64, 4096), dtype), pltpu.VMEM((*lead, 2, 256, 1024), dtype)]

    dma = pltpu.SemaphoreType.DMA
    any_space = pl.BlockSpec(memory_space=pl.ANY)

    def step(*arrays):
        out = pl.pallas_call(
            kernel,
            out_shape=[jax.ShapeDtypeStruct(s, BF16) for s in whole + block] + [jax.ShapeDtypeStruct((8, 128), F32)],
            in_specs=[any_space] * 12,
            out_specs=[any_space] * 6 + [pl.BlockSpec(memory_space=pltpu.VMEM)],
            scratch_shapes=[
                *pair((8,), BF16),
                *pair((3,), BF16),
                *pair((2,), BF16),
                *pair((), BF16),
                *pair((), F32),
                *pair((), F32),
                pltpu.VMEM((16, 1024), F32),
                pltpu.VMEM((16, 8, 128), F32),
                dma((8, 6)), dma((8, 6)), dma((3, 6)), dma((3, 6)), dma((2, 6)), dma((3, 6)),
                dma((7, 6)), dma((7, 6)), dma((16,)), dma((16,)), dma((6,)), dma((6,)),
            ],
            compiler_params=pltpu.CompilerParams(collective_id=0, has_side_effects=True, vmem_limit_bytes=66 * 1000 * 1000),
            name="step",
        )(*arrays)
        new_w, sums, factor = out[:3], out[3:6], out[6][0, 0]
        m, v = arrays[6:9], arrays[9:12]
        gs = [s.astype(F32) * factor for s in sums]
        return (*new_w, *(0.9 * a + 0.1 * b for a, b in zip(m, gs)), *(0.95 * a + 0.05 * b * b for a, b in zip(v, gs)))

    all_of, cut = P(None, None, None), P(None, "dp", None)
    return jax.shard_map(
        step,
        mesh=mesh,
        in_specs=(P(("rep", "dp"), None, None, None),) * 3 + (all_of,) * 3 + (cut,) * 6,
        out_specs=(P("rep", None, None),) * 3 + (P("rep", "dp", None),) * 6,
        check_vma=False,
    )
```

```python
import jax
import jax.numpy as jnp
from jax import lax
from jax.experimental import pallas as pl
from jax.experimental.pallas import tpu as pltpu
from jax.sharding import PartitionSpec as P


MESH = pl.DeviceIdType.MESH
F32 = jnp.float32
BF16 = jnp.bfloat16
CHIPS = 8
LAST = 6
CHUNKS = [(d, w) for w in range(3) for d in range(2)]


def device_at(q, c):
    y = q // 4
    z = q + y * (7 - 2 * q)
    return y * 8 + z * 2 + c


def tiles(ref, body):
    rows, cols = ref.shape

    def strip(r, carry):
        at = pl.ds(pl.multiple_of(r * 16, 16), 16)
        for k in range(cols // 1024):
            body(at, pl.ds(k * 1024, 1024))
        return carry

    lax.fori_loop(0, rows // 16, strip, 0)


def kernel(*refs):
    g, wt, m, v = (refs[i : i + 3] for i in (0, 3, 6, 9))
    x, gsum = refs[12:15], refs[15:18]
    factor_ref = refs[18]
    edge_gu, edge_dn = refs[19:21], refs[21:23]
    (p_gu, p_dn, r_gu, r_dn, o_gu, o_dn, w_gu, w_dn, m_gu, m_dn, v_gu, v_dn, acc, norms) = refs[23:37]
    (p_send, p_recv, r_send, r_recv, o_sem, state_sem, a_send, a_recv, n_send, n_recv, l_sem, g_sem) = refs[37:]

    rep, dp = lax.axis_index("rep"), lax.axis_index("dp")
    y, z, c = dp // 8, (dp // 2) % 4, dp % 2
    q = z + y * (7 - 2 * z)
    nxt = [(rep, device_at((q + 1) % CHIPS, c)), (rep, device_at((q + 7) % CHIPS, c))]
    partner = (rep, dp + 1 - 2 * c)

    def pick(gu, dn, lead, d, w):
        return gu.at[(*lead, d, w)] if w < 2 else dn.at[(*lead, d)]

    def rows_of(array, w, d, dev, lead=()):
        n = 64 if w < 2 else 256
        return array[w].at[(*lead, d, pl.ds(pl.multiple_of(dev * n, n), n), slice(None))]

    def scattered(s, d):
        return (q + 7 - s + CHIPS) % CHIPS if d == 0 else (q + 1 + s) % CHIPS

    def gathered(h, d):
        return (q + CHIPS - h) % CHIPS if d == 0 else (q + h) % CHIPS

    def own_load(s, d, w):
        return pltpu.make_async_copy(
            rows_of(g, w, d, device_at(scattered(s, d), c), (0,)), pick(o_gu, o_dn, (s % 2,), d, w), o_sem.at[s % 2, d * 3 + w]
        )

    def to_partner(s, d, w):
        return pltpu.make_async_remote_copy(
            rows_of(g, w, d, device_at(scattered(s, d), 1 - c), (0,)),
            pick(p_gu, p_dn, (s,), d, w),
            p_send.at[s, d * 3 + w],
            p_recv.at[s, d * 3 + w],
            device_id=partner,
            device_id_type=MESH,
        )

    def hop(s, d, w):
        return pltpu.make_async_remote_copy(
            pick(p_gu, p_dn, (s,), d, w),
            pick(r_gu, r_dn, (s % 3,), d, w),
            r_send.at[s % 3, d * 3 + w],
            r_recv.at[s % 3, d * 3 + w],
            device_id=nxt[d],
            device_id_type=MESH,
        )

    def state_loads(d, w):
        i = d * 3 + w
        return [
            pltpu.make_async_copy(m[w].at[d], pick(m_gu, m_dn, (), d, w), state_sem.at[0, i]),
            pltpu.make_async_copy(v[w].at[d], pick(v_gu, v_dn, (), d, w), state_sem.at[1, i]),
            pltpu.make_async_copy(rows_of(wt, w, d, dp), pick(w_gu, w_dn, (), d, w), state_sem.at[2, i]),
        ]

    barrier = pltpu.get_barrier_semaphore()
    for dev in (*nxt, partner):
        pl.semaphore_signal(barrier, inc=1, device_id=dev, device_id_type=MESH)
    for d, w in CHUNKS:
        own_load(0, d, w).start()
    pl.semaphore_wait(barrier, 3)
    for s in (0, 1):
        for d, w in CHUNKS:
            to_partner(s, d, w).start()

    def scatter_step(s, first, last):
        if not last:
            for d, w in CHUNKS:
                own_load(s + 1, d, w).start()
            if first:
                for d, w in CHUNKS:
                    to_partner(s + 2, d, w).start()
            else:

                @pl.when(s < 6)
                def _():
                    for d, w in CHUNKS:
                        to_partner(s + 2, d, w).start()

        for d, w in CHUNKS:
            own, theirs = pick(o_gu, o_dn, (s % 2,), d, w), pick(p_gu, p_dn, (s,), d, w)
            own_load(s, d, w).wait()
            to_partner(s, d, w).wait()
            if first:

                def add(rows, cols):
                    theirs[rows, cols] = (own[rows, cols].astype(F32) + theirs[rows, cols].astype(F32)).astype(BF16)

            else:
                before = (s + 2) % 3
                so_far = pick(r_gu, r_dn, (before,), d, w)
                hop(s - 1, d, w).wait_recv()

                def add(rows, cols):
                    total = (own[rows, cols].astype(F32) + theirs[rows, cols].astype(F32)) + so_far[rows, cols].astype(F32)
                    total = total.astype(BF16)
                    theirs[rows, cols] = total
                    if last:
                        acc[...] += total.astype(F32) * total.astype(F32)

            tiles(theirs, add)
            if last:
                pltpu.make_async_copy(theirs, gsum[w].at[d], g_sem.at[d * 3 + w]).start()
            else:
                if not first:

                    @pl.when(s >= 3)
                    def _():
                        hop(s - 3, d, w).wait_send()

                hop(s, d, w).start()

    scatter_step(0, True, False)
    for d, w in CHUNKS:
        for copy in state_loads(d, w):
            copy.start()
    acc[...] = jnp.zeros_like(acc)
    lax.fori_loop(1, 7, lambda s, carry: (scatter_step(s, False, False), carry)[1], 0)
    scatter_step(7, False, True)

    mine = acc[0:8, 0:128] + acc[8:16, 0:128]
    for k in range(1, 8):
        at = pl.ds(k * 128, 128)
        mine += acc[0:8, at] + acc[8:16, at]
    norms[dp] = mine

    def norm_to(r):
        return pltpu.make_async_remote_copy(
            norms.at[dp], norms.at[dp], n_send.at[r], n_recv.at[dp], device_id=(rep, (dp + r) % 16), device_id_type=MESH
        )

    def norm_from(r):
        src = (dp + 16 - r) % 16
        return pltpu.make_async_remote_copy(
            norms.at[src], norms.at[src], n_send.at[r], n_recv.at[src], device_id=(rep, src), device_id_type=MESH
        )

    for r in range(1, 16):
        norm_to(r).start()
    for s in (4, 5, 6):
        for d, w in CHUNKS:
            hop(s, d, w).wait_send()
    for d, w in CHUNKS:
        for copy in state_loads(d, w):
            copy.wait()
    for r in range(1, 16):
        norm_from(r).wait_recv()
    squares = norms[0]
    for k in range(1, 16):
        squares += norms[k]
    count = 16 * 2 * (64 * 4096 * 2 + 256 * 1024)
    mean = jnp.sum(squares) * (1.0 / count)
    factor = jnp.minimum(1.0, 0.5 * lax.rsqrt(jnp.full((8, 128), mean, F32) + 1e-30))
    factor_ref[...] = factor
    scale = jnp.broadcast_to(factor[0:1, 0:1], (16, 1024))

    def edge(d, w):
        return edge_gu[d].at[w] if w < 2 else edge_dn[d]

    def held(h, d, w):
        if isinstance(h, int) and h == 0:
            return pick(p_gu, p_dn, (0,), d, w)
        if isinstance(h, int) and h == LAST:
            return edge(d, w)
        return rows_of(x, w, d, device_at(gathered(h, d), c))

    def gather_hop(h, d, w):
        dst = edge(d, w) if isinstance(h, int) and h == LAST - 1 else rows_of(x, w, d, device_at(gathered(h, d), c))
        return pltpu.make_async_remote_copy(
            held(h, d, w), dst, a_send.at[h, d * 3 + w], a_recv.at[h, d * 3 + w], device_id=nxt[d], device_id_type=MESH
        )

    def gather_from(h, d, w):
        block = held(h, d, w)
        return pltpu.make_async_remote_copy(
            block, block, a_send.at[h - 1, d * 3 + w], a_recv.at[h - 1, d * 3 + w], device_id=nxt[d], device_id_type=MESH
        )

    def share(h, d, w):
        return pltpu.make_async_remote_copy(
            held(h, d, w),
            rows_of(x, w, d, device_at(gathered(h, d), c)),
            p_send.at[h, d * 3 + w],
            p_recv.at[h, d * 3 + w],
            device_id=partner,
            device_id_type=MESH,
        )

    def shared(h, d, w):
        block = rows_of(x, w, d, device_at(gathered(h, d), 1 - c))
        return pltpu.make_async_remote_copy(
            block, block, p_send.at[h, d * 3 + w], p_recv.at[h, d * 3 + w], device_id=partner, device_id_type=MESH
        )

    def keep(d, w):
        return pltpu.make_async_copy(pick(p_gu, p_dn, (0,), d, w), rows_of(x, w, d, dp), l_sem.at[d * 3 + w])

    for d, w in CHUNKS:
        gr, new = pick(p_gu, p_dn, (7,), d, w), pick(p_gu, p_dn, (0,), d, w)
        mr, vr, wr = pick(m_gu, m_dn, (), d, w), pick(v_gu, v_dn, (), d, w), pick(w_gu, w_dn, (), d, w)

        def update(rows, cols):
            grad = gr[rows, cols].astype(F32) * scale
            m1 = 0.9 * mr[rows, cols] + 0.1 * grad
            v1 = 0.95 * vr[rows, cols] + 0.05 * grad * grad
            old = wr[rows, cols].astype(F32)
            new[rows, cols] = (old - 0.02 * (m1 * lax.rsqrt(v1 + 1e-8) + 0.1 * old)).astype(BF16)

        tiles(new, update)
        gather_hop(0, d, w).start()
        share(0, d, w).start()
        keep(d, w).start()

    def gather_step(h, carry):
        for d, w in CHUNKS:
            gather_from(h, d, w).wait_recv()
            gather_hop(h, d, w).start()
            share(h, d, w).start()
        return carry

    lax.fori_loop(1, LAST - 1, gather_step, 0)
    gather_step(LAST - 1, 0)
    for d, w in CHUNKS:
        gather_from(LAST, d, w).wait_recv()
        share(LAST, d, w).start()

    for r in range(1, 16):
        norm_to(r).wait_send()
    for d, w in CHUNKS:
        keep(d, w).wait()
        pltpu.make_async_copy(pick(p_gu, p_dn, (7,), d, w), gsum[w].at[d], g_sem.at[d * 3 + w]).wait()

    def drain(h, carry):
        for d, w in CHUNKS:
            gather_from(h + 1, d, w).wait_send()
        return carry

    lax.fori_loop(0, LAST, drain, 0)

    def drain_shares(h, carry):
        for d, w in CHUNKS:
            shared(h, d, w).wait()
        return carry

    lax.fori_loop(0, LAST + 1, drain_shares, 0)


def place():
    dp = lax.axis_index("dp")
    y, z, c = dp // 8, (dp // 2) % 4, dp % 2
    return dp, z + y * (7 - 2 * z), c


def block_rows(array, d, dev, count=1):
    n = array.shape[1] // 16
    return array.at[d, pl.ds(pl.multiple_of(dev * n, n), n * count)]


def from_chip(q, h, d):
    return (q + CHIPS - h) % CHIPS if d == 0 else (q + h) % CHIPS


def arrived(x, edges, out):
    _, q, c = place()
    pairs = []
    for d in range(2):
        for h in range(LAST):
            chip = device_at(from_chip(q, h, d), 0)
            pairs.append((block_rows(x, d, chip, 2), block_rows(out, d, chip, 2)))
        chip = from_chip(q, LAST, d)
        pairs.append((edges[d], block_rows(out, d, device_at(chip, c))))
        other = device_at(chip, 1 - c)
        pairs.append((block_rows(x, d, other), block_rows(out, d, other)))
    return pairs


def through(pairs, slots, in_sem, out_sem):
    loads, stores = [], []
    for i, (src, dst) in enumerate(pairs):
        at = slots.at[i % 16, pl.ds(0, src.shape[0])]
        loads.append(pltpu.make_async_copy(src, at, in_sem.at[i % 16]))
        stores.append(pltpu.make_async_copy(at, dst, out_sem.at[i % 16]))
    n = len(pairs)
    for i in range(min(8, n)):
        loads[i].start()
    for i in range(n):
        loads[i].wait()
        stores[i].start()
        if i >= 8:
            stores[i - 8].wait()
        if i + 8 < n:
            loads[i + 8].start()
    for i in range(max(0, n - 8), n):
        stores[i].wait()


def copy_wide(xg, xu, e0, e1, out_g, out_u, slots, in_sem, out_sem):
    pairs = []
    for w, (x, out) in enumerate(((xg, out_g), (xu, out_u))):
        pairs += arrived(x, [e0.at[w], e1.at[w]], out)
    through(pairs, slots, in_sem, out_sem)


def copy_down(*refs):
    factor, x, e0, e1 = refs[:4]
    gs, ms, vs = refs[4:7], refs[7:10], refs[10:13]
    out, m_out, v_out = refs[13], refs[14:17], refs[17:20]
    slots, g_gu, g_dn, m_gu, m_dn, v_gu, v_dn, in_sem, out_sem, state_in, state_out = refs[20:]

    def pick(gu, dn, d, w):
        return gu.at[d, w] if w < 2 else dn.at[d]

    def load(d, w):
        i = d * 3 + w
        return [
            pltpu.make_async_copy(gs[w].at[d], pick(g_gu, g_dn, d, w), state_in.at[0, i]),
            pltpu.make_async_copy(ms[w].at[d], pick(m_gu, m_dn, d, w), state_in.at[1, i]),
            pltpu.make_async_copy(vs[w].at[d], pick(v_gu, v_dn, d, w), state_in.at[2, i]),
        ]

    def store(d, w):
        i = d * 3 + w
        return [
            pltpu.make_async_copy(pick(m_gu, m_dn, d, w), m_out[w].at[d], state_out.at[0, i]),
            pltpu.make_async_copy(pick(v_gu, v_dn, d, w), v_out[w].at[d], state_out.at[1, i]),
        ]

    for d, w in CHUNKS:
        for one in load(d, w):
            one.start()
    scale = jnp.broadcast_to(factor[0:1, 0:1], (16, 1024))
    for d, w in CHUNKS:
        for one in load(d, w):
            one.wait()
        gr, mr, vr = pick(g_gu, g_dn, d, w), pick(m_gu, m_dn, d, w), pick(v_gu, v_dn, d, w)

        def update(rows, cols):
            grad = gr[rows, cols].astype(F32) * scale
            mr[rows, cols] = 0.9 * mr[rows, cols] + 0.1 * grad
            vr[rows, cols] = 0.95 * vr[rows, cols] + 0.05 * grad * grad

        tiles(gr, update)
        for one in store(d, w):
            one.start()
    through(arrived(x, [e0, e1], out), slots, in_sem, out_sem)
    for d, w in CHUNKS:
        for one in store(d, w):
            one.wait()


def finish(weights, *refs):
    lands = refs[weights : weights + 4]
    outs = refs[weights + 4 : 2 * weights + 4]
    slots, in_sem, out_sem = refs[2 * weights + 4 :]
    _, q, c = place()
    pairs = []
    for d in range(2):
        chip = from_chip(q, LAST + 1, d)
        for which in range(2):
            dev = device_at(chip, c if which == 0 else 1 - c)
            for w in range(weights):
                src = lands[which * 2 + d]
                pairs.append((src.at[w] if weights > 1 else src, block_rows(outs[w], d, dev)))
    through(pairs, slots, in_sem, out_sem)


def solution(mesh):
    whole = [(2, 1024, 4096), (2, 1024, 4096), (2, 4096, 1024)]
    block = [(2, 64, 4096), (2, 64, 4096), (2, 256, 1024)]

    def shapes(dims, dtype):
        return [jax.ShapeDtypeStruct(s, dtype) for s in dims]

    def pair(lead, dtype):
        return [pltpu.VMEM((*lead, 2, 2, 64, 4096), dtype), pltpu.VMEM((*lead, 2, 256, 1024), dtype)]

    dma = pltpu.SemaphoreType.DMA
    anywhere = pl.BlockSpec(memory_space=pl.ANY)
    hbm = pl.BlockSpec(memory_space=pltpu.HBM)
    vmem = pl.BlockSpec(memory_space=pltpu.VMEM)
    mib = 1024 * 1024

    def local(body, outs, ins, scratch, moved, aliases=None, specs=None):
        return call_local(body, outs, ins, scratch, moved, aliases, specs)

    def call_local(body, outs, ins, scratch, moved, aliases, specs):
        return pl.pallas_call(
            body,
            out_shape=outs,
            in_specs=specs or [hbm] * len(ins),
            out_specs=[hbm] * len(outs),
            scratch_shapes=scratch,
            input_output_aliases=aliases or {},
            cost_estimate=pl.CostEstimate(flops=int(moved * 40), bytes_accessed=int(moved), transcendentals=0),
            compiler_params=pltpu.CompilerParams(vmem_limit_bytes=48 * mib),
        )(*ins)

    def permute(array, pairs):
        return lax.ppermute(array, "dp", pairs)

    def at(q, c):
        return device_at(q % CHIPS, c)

    clockwise = [(at(q, c), at(q + 1, c)) for q in range(CHIPS) for c in range(2)]
    ways = [clockwise, [(b, a) for a, b in clockwise]]
    across = [(i, i ^ 1) for i in range(16)]

    def step(*arrays):
        m, v = arrays[6:9], arrays[9:12]
        out = pl.pallas_call(
            kernel,
            out_shape=[
                *shapes(whole + block, BF16),
                jax.ShapeDtypeStruct((8, 128), F32),
                *shapes([(2, 64, 4096)] * 2 + [(256, 1024)] * 2, BF16),
            ],
            in_specs=[hbm] * 12,
            out_specs=[hbm] * 6 + [vmem] + [hbm] * 4,
            scratch_shapes=[
                *pair((8,), BF16),
                *pair((3,), BF16),
                *pair((2,), BF16),
                *pair((), BF16),
                *pair((), F32),
                *pair((), F32),
                pltpu.VMEM((16, 1024), F32),
                pltpu.VMEM((16, 8, 128), F32),
                dma((8, 6)), dma((8, 6)), dma((3, 6)), dma((3, 6)), dma((2, 6)), dma((3, 6)),
                dma((7, 6)), dma((7, 6)), dma((16,)), dma((16,)), dma((6,)), dma((6,)),
            ],
            compiler_params=pltpu.CompilerParams(collective_id=0, has_side_effects=True, vmem_limit_bytes=66 * 1000 * 1000),
            name="step",
        )(*arrays)
        (xg, xu, xd), sums, factor, (e0, e1, f0, f1) = out[:3], out[3:6], out[6], out[7:]
        wide = [permute(e, ways[d]) for d, e in enumerate((e0, e1))]
        deep = [permute(e, ways[d]) for d, e in enumerate((f0, f1))]
        slots = [dma((16,)), dma((16,))]
        new_g, new_u = local(
            copy_wide, shapes(whole[:2], BF16), (xg, xu, e0, e1), [pltpu.VMEM((16, 128, 4096), BF16), *slots], 56 * mib
        )
        wide += [permute(e, across) for e in wide]
        new_d, *state = local(
            copy_down,
            shapes(whole[2:], BF16) + shapes(block * 2, F32),
            (factor, xd, f0, f1, *sums, *m, *v),
            [
                pltpu.VMEM((16, 512, 1024), BF16), *pair((), BF16), *pair((), F32), *pair((), F32),
                *slots, dma((3, 6)), dma((2, 6)),
            ],
            56 * mib,
            specs=[vmem] + [hbm] * 12,
        )
        deep += [permute(e, across) for e in deep]
        new_g, new_u = local(
            lambda *refs: finish(2, *refs),
            shapes(whole[:2], BF16),
            (new_g, new_u, *wide),
            [pltpu.VMEM((16, 64, 4096), BF16), *slots],
            8 * mib,
            {0: 0, 1: 1},
            [hbm] * 2 + [anywhere] * 4,
        )
        (new_d,) = local(
            lambda *refs: finish(1, *refs),
            shapes(whole[2:], BF16),
            (new_d, *deep),
            [pltpu.VMEM((16, 256, 1024), BF16), *slots],
            4 * mib,
            {0: 0},
            [hbm] + [anywhere] * 4,
        )
        return (new_g, new_u, new_d, *state)

    all_of, cut = P(None, None, None), P(None, "dp", None)
    return jax.shard_map(
        step,
        mesh=mesh,
        in_specs=(P(("rep", "dp"), None, None, None),) * 3 + (all_of,) * 3 + (cut,) * 6,
        out_specs=(P("rep", None, None),) * 3 + (P("rep", "dp", None),) * 6,
        check_vma=False,
    )
```

```python
import jax
import jax.numpy as jnp
from jax import lax
from jax.experimental import pallas as pl
from jax.experimental.pallas import tpu as pltpu
from jax.sharding import PartitionSpec as P


MESH = pl.DeviceIdType.MESH
F32 = jnp.float32
BF16 = jnp.bfloat16
CHIPS = 8
LAST = 5
CHUNKS = [(d, w) for w in range(3) for d in range(2)]


def device_at(q, c):
    y = q // 4
    z = q + y * (7 - 2 * q)
    return y * 8 + z * 2 + c


def tiles(ref, body):
    rows, cols = ref.shape

    def strip(r, carry):
        at = pl.ds(pl.multiple_of(r * 16, 16), 16)
        for k in range(cols // 1024):
            body(at, pl.ds(k * 1024, 1024))
        return carry

    lax.fori_loop(0, rows // 16, strip, 0)


def kernel(*refs):
    g, wt, m, v = (refs[i : i + 3] for i in (0, 3, 6, 9))
    x, gsum = refs[12:15], refs[15:18]
    factor_ref = refs[18]
    edge_gu, edge_dn = refs[19:21], refs[21:23]
    (p_gu, p_dn, r_gu, r_dn, o_gu, o_dn, w_gu, w_dn, m_gu, m_dn, v_gu, v_dn, acc, norms) = refs[23:37]
    (p_send, p_recv, r_send, r_recv, o_sem, state_sem, a_send, a_recv, n_send, n_recv, l_sem, g_sem) = refs[37:]

    rep, dp = lax.axis_index("rep"), lax.axis_index("dp")
    y, z, c = dp // 8, (dp // 2) % 4, dp % 2
    q = z + y * (7 - 2 * z)
    nxt = [(rep, device_at((q + 1) % CHIPS, c)), (rep, device_at((q + 7) % CHIPS, c))]
    partner = (rep, dp + 1 - 2 * c)

    def pick(gu, dn, lead, d, w):
        return gu.at[(*lead, d, w)] if w < 2 else dn.at[(*lead, d)]

    def rows_of(array, w, d, dev, lead=()):
        n = 64 if w < 2 else 256
        return array[w].at[(*lead, d, pl.ds(pl.multiple_of(dev * n, n), n), slice(None))]

    def scattered(s, d):
        return (q + 7 - s + CHIPS) % CHIPS if d == 0 else (q + 1 + s) % CHIPS

    def gathered(h, d):
        return (q + CHIPS - h) % CHIPS if d == 0 else (q + h) % CHIPS

    def own_load(s, d, w):
        return pltpu.make_async_copy(
            rows_of(g, w, d, device_at(scattered(s, d), c), (0,)), pick(o_gu, o_dn, (s % 2,), d, w), o_sem.at[s % 2, d * 3 + w]
        )

    def to_partner(s, d, w):
        return pltpu.make_async_remote_copy(
            rows_of(g, w, d, device_at(scattered(s, d), 1 - c), (0,)),
            pick(p_gu, p_dn, (s,), d, w),
            p_send.at[s, d * 3 + w],
            p_recv.at[s, d * 3 + w],
            device_id=partner,
            device_id_type=MESH,
        )

    def hop(s, d, w):
        return pltpu.make_async_remote_copy(
            pick(p_gu, p_dn, (s,), d, w),
            pick(r_gu, r_dn, (s % 3,), d, w),
            r_send.at[s % 3, d * 3 + w],
            r_recv.at[s % 3, d * 3 + w],
            device_id=nxt[d],
            device_id_type=MESH,
        )

    def state_loads(d, w):
        i = d * 3 + w
        return [
            pltpu.make_async_copy(m[w].at[d], pick(m_gu, m_dn, (), d, w), state_sem.at[0, i]),
            pltpu.make_async_copy(v[w].at[d], pick(v_gu, v_dn, (), d, w), state_sem.at[1, i]),
            pltpu.make_async_copy(rows_of(wt, w, d, dp), pick(w_gu, w_dn, (), d, w), state_sem.at[2, i]),
        ]

    barrier = pltpu.get_barrier_semaphore()
    for dev in (*nxt, partner):
        pl.semaphore_signal(barrier, inc=1, device_id=dev, device_id_type=MESH)
    for d, w in CHUNKS:
        own_load(0, d, w).start()
    pl.semaphore_wait(barrier, 3)
    for s in (0, 1):
        for d, w in CHUNKS:
            to_partner(s, d, w).start()

    def scatter_step(s, first, last):
        if not last:
            for d, w in CHUNKS:
                own_load(s + 1, d, w).start()
            if first:
                for d, w in CHUNKS:
                    to_partner(s + 2, d, w).start()
            else:

                @pl.when(s < 6)
                def _():
                    for d, w in CHUNKS:
                        to_partner(s + 2, d, w).start()

        for d, w in CHUNKS:
            own, theirs = pick(o_gu, o_dn, (s % 2,), d, w), pick(p_gu, p_dn, (s,), d, w)
            own_load(s, d, w).wait()
            to_partner(s, d, w).wait()
            if first:

                def add(rows, cols):
                    theirs[rows, cols] = (own[rows, cols].astype(F32) + theirs[rows, cols].astype(F32)).astype(BF16)

            else:
                before = (s + 2) % 3
                so_far = pick(r_gu, r_dn, (before,), d, w)
                hop(s - 1, d, w).wait_recv()

                def add(rows, cols):
                    total = (own[rows, cols].astype(F32) + theirs[rows, cols].astype(F32)) + so_far[rows, cols].astype(F32)
                    total = total.astype(BF16)
                    theirs[rows, cols] = total
                    if last:
                        acc[...] += total.astype(F32) * total.astype(F32)

            tiles(theirs, add)
            if last:
                pltpu.make_async_copy(theirs, gsum[w].at[d], g_sem.at[d * 3 + w]).start()
            else:
                if not first:

                    @pl.when(s >= 3)
                    def _():
                        hop(s - 3, d, w).wait_send()

                hop(s, d, w).start()

    scatter_step(0, True, False)
    for d, w in CHUNKS:
        for copy in state_loads(d, w):
            copy.start()
    acc[...] = jnp.zeros_like(acc)
    lax.fori_loop(1, 7, lambda s, carry: (scatter_step(s, False, False), carry)[1], 0)
    scatter_step(7, False, True)

    mine = acc[0:8, 0:128] + acc[8:16, 0:128]
    for k in range(1, 8):
        at = pl.ds(k * 128, 128)
        mine += acc[0:8, at] + acc[8:16, at]
    norms[dp] = mine

    def norm_to(r):
        return pltpu.make_async_remote_copy(
            norms.at[dp], norms.at[dp], n_send.at[r], n_recv.at[dp], device_id=(rep, (dp + r) % 16), device_id_type=MESH
        )

    def norm_from(r):
        src = (dp + 16 - r) % 16
        return pltpu.make_async_remote_copy(
            norms.at[src], norms.at[src], n_send.at[r], n_recv.at[src], device_id=(rep, src), device_id_type=MESH
        )

    for r in range(1, 16):
        norm_to(r).start()
    for s in (4, 5, 6):
        for d, w in CHUNKS:
            hop(s, d, w).wait_send()
    for d, w in CHUNKS:
        for copy in state_loads(d, w):
            copy.wait()
    for r in range(1, 16):
        norm_from(r).wait_recv()
    squares = norms[0]
    for k in range(1, 16):
        squares += norms[k]
    count = 16 * 2 * (64 * 4096 * 2 + 256 * 1024)
    mean = jnp.sum(squares) * (1.0 / count)
    factor = jnp.minimum(1.0, 0.5 * lax.rsqrt(jnp.full((8, 128), mean, F32) + 1e-30))
    factor_ref[...] = factor
    scale = jnp.broadcast_to(factor[0:1, 0:1], (16, 1024))

    def edge(d, w):
        return edge_gu[d].at[w] if w < 2 else edge_dn[d]

    def held(h, d, w):
        if isinstance(h, int) and h == 0:
            return pick(p_gu, p_dn, (0,), d, w)
        if isinstance(h, int) and h == LAST:
            return edge(d, w)
        return rows_of(x, w, d, device_at(gathered(h, d), c))

    def gather_hop(h, d, w):
        dst = edge(d, w) if isinstance(h, int) and h == LAST - 1 else rows_of(x, w, d, device_at(gathered(h, d), c))
        return pltpu.make_async_remote_copy(
            held(h, d, w), dst, a_send.at[h, d * 3 + w], a_recv.at[h, d * 3 + w], device_id=nxt[d], device_id_type=MESH
        )

    def gather_from(h, d, w):
        block = held(h, d, w)
        return pltpu.make_async_remote_copy(
            block, block, a_send.at[h - 1, d * 3 + w], a_recv.at[h - 1, d * 3 + w], device_id=nxt[d], device_id_type=MESH
        )

    def share(h, d, w):
        return pltpu.make_async_remote_copy(
            held(h, d, w),
            rows_of(x, w, d, device_at(gathered(h, d), c)),
            p_send.at[h, d * 3 + w],
            p_recv.at[h, d * 3 + w],
            device_id=partner,
            device_id_type=MESH,
        )

    def shared(h, d, w):
        block = rows_of(x, w, d, device_at(gathered(h, d), 1 - c))
        return pltpu.make_async_remote_copy(
            block, block, p_send.at[h, d * 3 + w], p_recv.at[h, d * 3 + w], device_id=partner, device_id_type=MESH
        )

    def keep(d, w):
        return pltpu.make_async_copy(pick(p_gu, p_dn, (0,), d, w), rows_of(x, w, d, dp), l_sem.at[d * 3 + w])

    for d, w in CHUNKS:
        gr, new = pick(p_gu, p_dn, (7,), d, w), pick(p_gu, p_dn, (0,), d, w)
        mr, vr, wr = pick(m_gu, m_dn, (), d, w), pick(v_gu, v_dn, (), d, w), pick(w_gu, w_dn, (), d, w)

        def update(rows, cols):
            grad = gr[rows, cols].astype(F32) * scale
            m1 = 0.9 * mr[rows, cols] + 0.1 * grad
            v1 = 0.95 * vr[rows, cols] + 0.05 * grad * grad
            old = wr[rows, cols].astype(F32)
            new[rows, cols] = (old - 0.02 * (m1 * lax.rsqrt(v1 + 1e-8) + 0.1 * old)).astype(BF16)

        tiles(new, update)
        gather_hop(0, d, w).start()
        share(0, d, w).start()
        keep(d, w).start()

    def gather_step(h, carry):
        for d, w in CHUNKS:
            gather_from(h, d, w).wait_recv()
            gather_hop(h, d, w).start()
            share(h, d, w).start()
        return carry

    lax.fori_loop(1, LAST - 1, gather_step, 0)
    gather_step(LAST - 1, 0)
    for d, w in CHUNKS:
        gather_from(LAST, d, w).wait_recv()

    for r in range(1, 16):
        norm_to(r).wait_send()
    for d, w in CHUNKS:
        keep(d, w).wait()
        pltpu.make_async_copy(pick(p_gu, p_dn, (7,), d, w), gsum[w].at[d], g_sem.at[d * 3 + w]).wait()

    def drain(h, carry):
        for d, w in CHUNKS:
            gather_from(h + 1, d, w).wait_send()
        return carry

    lax.fori_loop(0, LAST, drain, 0)

    def drain_shares(h, carry):
        for d, w in CHUNKS:
            shared(h, d, w).wait()
        return carry

    lax.fori_loop(0, LAST, drain_shares, 0)


def place():
    dp = lax.axis_index("dp")
    y, z, c = dp // 8, (dp // 2) % 4, dp % 2
    return dp, z + y * (7 - 2 * z), c


def block_rows(array, d, dev, count=1):
    n = array.shape[1] // 16
    return array.at[d, pl.ds(pl.multiple_of(dev * n, n), n * count)]


def from_chip(q, h, d):
    return (q + CHIPS - h) % CHIPS if d == 0 else (q + h) % CHIPS


def arrived(x, out):
    _, q, _ = place()
    chips = [(d, device_at(from_chip(q, h, d), 0)) for d in range(2) for h in range(LAST)]
    return [(block_rows(x, d, chip, 2), block_rows(out, d, chip, 2)) for d, chip in chips]


def landed(hop, lands, outs):
    _, q, c = place()
    pairs = []
    for i, land in enumerate(lands):
        dev = device_at(from_chip(q, hop, i % 2), c if i < 2 else 1 - c)
        for w, out in enumerate(outs):
            pairs.append((land.at[w] if len(outs) > 1 else land, block_rows(out, i % 2, dev)))
    return pairs


def through(pairs, slots, in_sem, out_sem):
    loads, stores = [], []
    for i, (src, dst) in enumerate(pairs):
        at = slots.at[i % 16, pl.ds(0, src.shape[0])]
        loads.append(pltpu.make_async_copy(src, at, in_sem.at[i % 16]))
        stores.append(pltpu.make_async_copy(at, dst, out_sem.at[i % 16]))
    n = len(pairs)
    for i in range(min(8, n)):
        loads[i].start()
    for i in range(n):
        loads[i].wait()
        stores[i].start()
        if i >= 8:
            stores[i - 8].wait()
        if i + 8 < n:
            loads[i + 8].start()
    for i in range(max(0, n - 8), n):
        stores[i].wait()


def copy_wide(xg, xu, out_g, out_u, slots, in_sem, out_sem):
    through(arrived(xg, out_g) + arrived(xu, out_u), slots, in_sem, out_sem)


def copy_down(*refs):
    factor, x = refs[:2]
    gs, ms, vs = refs[2:5], refs[5:8], refs[8:11]
    out, m_out, v_out = refs[11], refs[12:15], refs[15:18]
    slots, g_gu, g_dn, m_gu, m_dn, v_gu, v_dn, in_sem, out_sem, state_in, state_out = refs[18:]

    def pick(gu, dn, d, w):
        return gu.at[d, w] if w < 2 else dn.at[d]

    def load(d, w):
        i = d * 3 + w
        return [
            pltpu.make_async_copy(gs[w].at[d], pick(g_gu, g_dn, d, w), state_in.at[0, i]),
            pltpu.make_async_copy(ms[w].at[d], pick(m_gu, m_dn, d, w), state_in.at[1, i]),
            pltpu.make_async_copy(vs[w].at[d], pick(v_gu, v_dn, d, w), state_in.at[2, i]),
        ]

    def store(d, w):
        i = d * 3 + w
        return [
            pltpu.make_async_copy(pick(m_gu, m_dn, d, w), m_out[w].at[d], state_out.at[0, i]),
            pltpu.make_async_copy(pick(v_gu, v_dn, d, w), v_out[w].at[d], state_out.at[1, i]),
        ]

    for d, w in CHUNKS:
        for one in load(d, w):
            one.start()
    scale = jnp.broadcast_to(factor[0:1, 0:1], (16, 1024))
    for d, w in CHUNKS:
        for one in load(d, w):
            one.wait()
        gr, mr, vr = pick(g_gu, g_dn, d, w), pick(m_gu, m_dn, d, w), pick(v_gu, v_dn, d, w)

        def update(rows, cols):
            grad = gr[rows, cols].astype(F32) * scale
            mr[rows, cols] = 0.9 * mr[rows, cols] + 0.1 * grad
            vr[rows, cols] = 0.95 * vr[rows, cols] + 0.05 * grad * grad

        tiles(gr, update)
        for one in store(d, w):
            one.start()
    through(arrived(x, out), slots, in_sem, out_sem)
    for d, w in CHUNKS:
        for one in store(d, w):
            one.wait()


def settle(*refs):
    lands, outs, (wide_slots, down_slots, in_sem, out_sem) = refs[3:19], refs[19:22], refs[22:]
    wide = landed(LAST, lands[0:4], outs[:2]) + landed(LAST + 1, lands[4:8], outs[:2])
    down = landed(LAST, lands[8:12], outs[2:]) + landed(LAST + 1, lands[12:16], outs[2:])
    through(wide, wide_slots, in_sem, out_sem)
    through(down, down_slots, in_sem, out_sem)


def finish(weights, *refs):
    lands, outs, sem = refs[weights : weights + 4], refs[weights + 4 : 2 * weights + 4], refs[-1]
    copies = [pltpu.make_async_copy(src, dst, sem.at[i]) for i, (src, dst) in enumerate(landed(LAST + 2, lands, outs))]
    for copy in copies:
        copy.start()
    for copy in copies:
        copy.wait()


def solution(mesh):
    whole = [(2, 1024, 4096), (2, 1024, 4096), (2, 4096, 1024)]
    block = [(2, 64, 4096), (2, 64, 4096), (2, 256, 1024)]

    def shapes(dims, dtype):
        return [jax.ShapeDtypeStruct(s, dtype) for s in dims]

    def pair(lead, dtype):
        return [pltpu.VMEM((*lead, 2, 2, 64, 4096), dtype), pltpu.VMEM((*lead, 2, 256, 1024), dtype)]

    dma = pltpu.SemaphoreType.DMA
    anywhere = pl.BlockSpec(memory_space=pl.ANY)
    hbm = pl.BlockSpec(memory_space=pltpu.HBM)
    vmem = pl.BlockSpec(memory_space=pltpu.VMEM)
    mib = 1024 * 1024

    def local(body, outs, ins, scratch, moved, limit, aliases=None, specs=None):
        return call_local(body, outs, ins, scratch, moved, limit, aliases, specs)

    def call_local(body, outs, ins, scratch, moved, limit, aliases, specs):
        return pl.pallas_call(
            body,
            out_shape=outs,
            in_specs=specs or [hbm] * len(ins),
            out_specs=[hbm] * len(outs),
            scratch_shapes=scratch,
            input_output_aliases=aliases or {},
            cost_estimate=pl.CostEstimate(flops=int(moved * 40), bytes_accessed=int(moved), transcendentals=0),
            compiler_params=pltpu.CompilerParams(vmem_limit_bytes=limit * mib),
        )(*ins)

    def permute(array, pairs):
        return lax.ppermute(array, "dp", pairs)

    def at(q, c):
        return device_at(q % CHIPS, c)

    clockwise = [(at(q, c), at(q + 1, c)) for q in range(CHIPS) for c in range(2)]
    ways = [clockwise, [(b, a) for a, b in clockwise]]
    across = [(i, i ^ 1) for i in range(16)]

    def step(*arrays):
        m, v = arrays[6:9], arrays[9:12]
        out = pl.pallas_call(
            kernel,
            out_shape=[
                *shapes(whole + block, BF16),
                jax.ShapeDtypeStruct((8, 128), F32),
                *shapes([(2, 64, 4096)] * 2 + [(256, 1024)] * 2, BF16),
            ],
            in_specs=[hbm] * 12,
            out_specs=[hbm] * 6 + [vmem] + [hbm] * 4,
            scratch_shapes=[
                *pair((8,), BF16),
                *pair((3,), BF16),
                *pair((2,), BF16),
                *pair((), BF16),
                *pair((), F32),
                *pair((), F32),
                pltpu.VMEM((16, 1024), F32),
                pltpu.VMEM((16, 8, 128), F32),
                dma((8, 6)), dma((8, 6)), dma((3, 6)), dma((3, 6)), dma((2, 6)), dma((3, 6)),
                dma((7, 6)), dma((7, 6)), dma((16,)), dma((16,)), dma((6,)), dma((6,)),
            ],
            compiler_params=pltpu.CompilerParams(collective_id=0, has_side_effects=True, vmem_limit_bytes=66 * 1000 * 1000),
            name="step",
        )(*arrays)
        (xg, xu, xd), sums, factor, (e0, e1, f0, f1) = out[:3], out[3:6], out[6], out[7:]
        slots = [dma((16,)), dma((16,))]

        def hop_on(arrays):
            return [permute(e, ways[d]) for d, e in enumerate(arrays)]

        def cross(arrays):
            return [permute(e, across) for e in arrays]

        wide5, deep5 = [e0, e1], [f0, f1]
        wide6, deep6 = hop_on(wide5), hop_on(deep5)
        their_wide5, their_deep5 = cross(wide5), cross(deep5)
        new_g, new_u = local(
            copy_wide, shapes(whole[:2], BF16), (xg, xu), [pltpu.VMEM((16, 128, 4096), BF16), *slots], 40 * mib, 50
        )
        wide7, their_wide6 = hop_on(wide6), cross(wide6)
        new_d, *state = local(
            copy_down,
            shapes(whole[2:], BF16) + shapes(block * 2, F32),
            (factor, xd, *sums, *m, *v),
            [
                pltpu.VMEM((16, 512, 1024), BF16), *pair((), BF16), *pair((), F32), *pair((), F32),
                *slots, dma((3, 6)), dma((2, 6)),
            ],
            48 * mib,
            50,
            specs=[vmem] + [hbm] * 10,
        )
        deep7, their_deep6 = hop_on(deep6), cross(deep6)
        news = local(
            settle,
            shapes(whole, BF16),
            (new_g, new_u, new_d, *wide5, *their_wide5, *wide6, *their_wide6, *deep5, *their_deep5, *deep6, *their_deep6),
            [pltpu.VMEM((16, 64, 4096), BF16), pltpu.VMEM((16, 256, 1024), BF16), *slots],
            24 * mib,
            24,
            {0: 0, 1: 1, 2: 2},
            [hbm] * 3 + [anywhere] * 16,
        )
        their_wide7 = cross(wide7)
        new_g, new_u = local(
            lambda *refs: finish(2, *refs), shapes(whole[:2], BF16), (*news[:2], *wide7, *their_wide7), [dma((8,))],
            8 * mib, 24, {0: 0, 1: 1}, [hbm] * 2 + [anywhere] * 4,
        )
        their_deep7 = cross(deep7)
        (new_d,) = local(
            lambda *refs: finish(1, *refs), shapes(whole[2:], BF16), (news[2], *deep7, *their_deep7), [dma((8,))],
            4 * mib, 24, {0: 0}, [hbm] + [anywhere] * 4,
        )
        return (new_g, new_u, new_d, *state)

    all_of, cut = P(None, None, None), P(None, "dp", None)
    return jax.shard_map(
        step,
        mesh=mesh,
        in_specs=(P(("rep", "dp"), None, None, None),) * 3 + (all_of,) * 3 + (cut,) * 6,
        out_specs=(P("rep", None, None),) * 3 + (P("rep", "dp", None),) * 6,
        check_vma=False,
    )
```

```python
import jax
import jax.numpy as jnp
from jax import lax
from jax.experimental import pallas as pl
from jax.experimental.pallas import tpu as pltpu
from jax.sharding import PartitionSpec as P


MESH = pl.DeviceIdType.MESH
F32 = jnp.float32
BF16 = jnp.bfloat16
CHIPS = 8
LAST = 5
BLOCKS = [(d, w) for w in range(3) for d in range(2)]
CHUNKS = [(d, w, j) for w in range(3) for j in range(2) for d in range(2)]


def device_at(q, c):
    y = q // 4
    z = q + y * (7 - 2 * q)
    return y * 8 + z * 2 + c


def tiles(ref, body):
    rows, cols = ref.shape

    def strip(r, carry):
        at = pl.ds(pl.multiple_of(r * 16, 16), 16)
        for k in range(cols // 1024):
            body(at, pl.ds(k * 1024, 1024))
        return carry

    lax.fori_loop(0, rows // 16, strip, 0)


def kernel(*refs):
    g, wt, m, v = (refs[i : i + 3] for i in (0, 3, 6, 9))
    x, gsum = refs[12:15], refs[15:18]
    factor_ref = refs[18]
    edge_gu, edge_dn = refs[19:21], refs[21:23]
    (p_gu, p_dn, r_gu, r_dn, o_gu, o_dn, w_gu, w_dn, m_gu, m_dn, v_gu, v_dn, acc, norms) = refs[23:37]
    (p_send, p_first, p_recv, r_send, r_recv, o_sem, state_sem, a_send, s_send, s_recv, n_send, n_recv, l_sem, g_sem) = refs[37:]

    rep, dp = lax.axis_index("rep"), lax.axis_index("dp")
    y, z, c = dp // 8, (dp // 2) % 4, dp % 2
    q = z + y * (7 - 2 * z)
    nxt = [(rep, device_at((q + 1) % CHIPS, c)), (rep, device_at((q + 7) % CHIPS, c))]
    partner = (rep, dp + 1 - 2 * c)

    def half(w, j, start=0):
        n = 32 if w < 2 else 128
        if j is None:
            return pl.ds(start, 2 * n)
        return pl.ds(start + j * n, n)

    def pick(gu, dn, lead, d, w, j=None):
        return gu.at[(*lead, d, w, half(w, j))] if w < 2 else dn.at[(*lead, d, half(w, j))]

    def rows_of(array, w, d, dev, lead=(), j=None):
        n = 64 if w < 2 else 256
        return array[w].at[(*lead, d, half(w, j, pl.multiple_of(dev * n, n)), slice(None))]

    def flag(d, w, j):
        return (d * 3 + w) * 2 + j

    def scattered(s, d):
        return (q + 7 - s + CHIPS) % CHIPS if d == 0 else (q + 1 + s) % CHIPS

    def gathered(h, d):
        return (q + CHIPS - h) % CHIPS if d == 0 else (q + h) % CHIPS

    def whole(gu, dn, sem, *lead):
        for i, part in enumerate((gu, dn)):
            ref = part.at[lead] if lead else part
            pltpu.make_async_copy(ref, ref, sem.at[i]).wait()

    def own_load(s, d, w):
        return pltpu.make_async_copy(
            rows_of(g, w, d, device_at(scattered(s, d), c), (0,)), pick(o_gu, o_dn, (s % 2,), d, w), o_sem.at[s % 2, w // 2]
        )

    def to_partner(s, d, w, j):
        return pltpu.make_async_remote_copy(
            rows_of(g, w, d, device_at(scattered(s, d), 1 - c), (0,), j),
            pick(p_gu, p_dn, (s,), d, w, j),
            p_send.at[w // 2],
            p_first.at[flag(d, w, j)] if isinstance(s, int) and s == 0 else p_recv.at[s, w // 2],
            device_id=partner,
            device_id_type=MESH,
        )

    def hop(s, d, w, j):
        return pltpu.make_async_remote_copy(
            pick(p_gu, p_dn, (s,), d, w, j),
            pick(r_gu, r_dn, (s % 3,), d, w, j),
            r_send.at[w // 2],
            r_recv.at[s % 3, flag(d, w, j)],
            device_id=nxt[d],
            device_id_type=MESH,
        )

    def state_loads(d, w):
        return [
            pltpu.make_async_copy(m[w].at[d], pick(m_gu, m_dn, (), d, w), state_sem.at[0, w // 2]),
            pltpu.make_async_copy(v[w].at[d], pick(v_gu, v_dn, (), d, w), state_sem.at[1, w // 2]),
            pltpu.make_async_copy(rows_of(wt, w, d, dp), pick(w_gu, w_dn, (), d, w), state_sem.at[2, w // 2]),
        ]

    def sum_out(d, w):
        return pltpu.make_async_copy(pick(p_gu, p_dn, (7,), d, w), gsum[w].at[d], g_sem.at[w // 2])

    barrier = pltpu.get_barrier_semaphore()
    for dev in (*nxt, partner):
        pl.semaphore_signal(barrier, inc=1, device_id=dev, device_id_type=MESH)
    for d, w in BLOCKS:
        own_load(0, d, w).start()
    pl.semaphore_wait(barrier, 3)
    for s in (0, 1):
        for d, w, j in CHUNKS:
            to_partner(s, d, w, j).start()

    def scatter_step(s, first, last):
        if not last:
            for d, w in BLOCKS:
                own_load(s + 1, d, w).start()
            if first:
                for d, w, j in CHUNKS:
                    to_partner(s + 2, d, w, j).start()
            else:

                @pl.when(s < 6)
                def _():
                    for d, w, j in CHUNKS:
                        to_partner(s + 2, d, w, j).start()

        whole(o_gu, o_dn, o_sem.at[s % 2], s % 2)
        if not first:
            whole(p_gu, p_dn, p_recv.at[s], s)
        for d, w, j in CHUNKS:
            own, theirs = pick(o_gu, o_dn, (s % 2,), d, w, j), pick(p_gu, p_dn, (s,), d, w, j)
            if first:
                to_partner(s, d, w, j).wait_recv()

                def add(rows, cols):
                    theirs[rows, cols] = (own[rows, cols].astype(F32) + theirs[rows, cols].astype(F32)).astype(BF16)

            else:
                before = (s + 2) % 3
                so_far = pick(r_gu, r_dn, (before,), d, w, j)
                hop(s - 1, d, w, j).wait_recv()

                def add(rows, cols):
                    total = (own[rows, cols].astype(F32) + theirs[rows, cols].astype(F32)) + so_far[rows, cols].astype(F32)
                    total = total.astype(BF16)
                    theirs[rows, cols] = total
                    if last:
                        acc[...] += total.astype(F32) * total.astype(F32)

            tiles(theirs, add)
            if last:
                if j == 1:
                    sum_out(d, w).start()
            else:
                hop(s, d, w, j).start()

    scatter_step(0, True, False)
    for d, w in BLOCKS:
        for copy in state_loads(d, w):
            copy.start()
    acc[...] = jnp.zeros_like(acc)
    lax.fori_loop(1, 7, lambda s, carry: (scatter_step(s, False, False), carry)[1], 0)
    scatter_step(7, False, True)

    mine = acc[0:8, 0:128] + acc[8:16, 0:128]
    for k in range(1, 8):
        at = pl.ds(k * 128, 128)
        mine += acc[0:8, at] + acc[8:16, at]
    norms[dp] = jnp.sum(mine, axis=0, keepdims=True)
    for r in range(1, 16):
        pltpu.make_async_remote_copy(
            norms.at[dp], norms.at[dp], n_send.at[0], n_recv.at[0], device_id=(rep, (dp + r) % 16), device_id_type=MESH
        ).start()
    whole(p_gu, p_dn, r_send, pl.ds(0, 7))
    whole(p_gu, p_dn, p_send)
    for i, (gu, dn) in enumerate(((m_gu, m_dn), (v_gu, v_dn), (w_gu, w_dn))):
        whole(gu, dn, state_sem.at[i])
    others = norms.at[pl.ds(0, 15)]
    pltpu.make_async_copy(others, others, n_send.at[0]).wait()
    pltpu.make_async_copy(others, others, n_recv.at[0]).wait()
    squares = norms[0]
    for k in range(1, 16):
        squares += norms[k]
    count = 16 * 2 * (64 * 4096 * 2 + 256 * 1024)
    mean = jnp.sum(squares) * (1.0 / count)
    factor = jnp.minimum(1.0, 0.5 * lax.rsqrt(jnp.full((8, 128), mean, F32) + 1e-30))
    factor_ref[...] = factor
    scale = jnp.broadcast_to(factor[0:1, 0:1], (16, 1024))

    def edge(d, w, j):
        return edge_gu[d].at[w, half(w, j)] if w < 2 else edge_dn[d].at[half(w, j)]

    def held(h, d, w, j):
        if isinstance(h, int) and h == 0:
            return pick(p_gu, p_dn, (0,), d, w, j)
        if isinstance(h, int) and h == LAST:
            return edge(d, w, j)
        return rows_of(x, w, d, device_at(gathered(h, d), c), (), j)

    def gather_hop(h, d, w, j):
        dst = edge(d, w, j) if isinstance(h, int) and h == LAST - 1 else rows_of(x, w, d, device_at(gathered(h, d), c), (), j)
        return pltpu.make_async_remote_copy(
            held(h, d, w, j), dst, a_send.at[w // 2], r_recv.at[(h + 1) % 3, flag(d, w, j)], device_id=nxt[d], device_id_type=MESH
        )

    def gather_from(h, d, w, j):
        block = held(h, d, w, j)
        return pltpu.make_async_remote_copy(
            block, block, a_send.at[w // 2], r_recv.at[h % 3, flag(d, w, j)], device_id=nxt[d], device_id_type=MESH
        )

    def share(h, d, w, j):
        return pltpu.make_async_remote_copy(
            held(h, d, w, j),
            rows_of(x, w, d, device_at(gathered(h, d), c), (), j),
            s_send.at[w // 2],
            s_recv.at[w // 2],
            device_id=partner,
            device_id_type=MESH,
        )

    def keep(d, w):
        return pltpu.make_async_copy(pick(p_gu, p_dn, (0,), d, w), rows_of(x, w, d, dp), l_sem.at[w // 2])

    for d, w, j in CHUNKS:
        gr, new = pick(p_gu, p_dn, (7,), d, w, j), pick(p_gu, p_dn, (0,), d, w, j)
        mr, vr, wr = pick(m_gu, m_dn, (), d, w, j), pick(v_gu, v_dn, (), d, w, j), pick(w_gu, w_dn, (), d, w, j)

        def update(rows, cols):
            grad = gr[rows, cols].astype(F32) * scale
            m1 = 0.9 * mr[rows, cols] + 0.1 * grad
            v1 = 0.95 * vr[rows, cols] + 0.05 * grad * grad
            old = wr[rows, cols].astype(F32)
            new[rows, cols] = (old - 0.02 * (m1 * lax.rsqrt(v1 + 1e-8) + 0.1 * old)).astype(BF16)

        tiles(new, update)
        gather_hop(0, d, w, j).start()
        share(0, d, w, j).start()
        if j == 1:
            keep(d, w).start()

    def gather_step(h, carry):
        for d, w, j in CHUNKS:
            gather_from(h, d, w, j).wait_recv()
            gather_hop(h, d, w, j).start()
            share(h, d, w, j).start()
        return carry

    lax.fori_loop(1, LAST - 1, gather_step, 0)
    gather_step(LAST - 1, 0)
    whole(p_gu, p_dn, l_sem, 0)
    whole(p_gu, p_dn, g_sem, 7)
    whole(p_gu, p_dn, s_send, pl.ds(0, LAST))
    whole(p_gu, p_dn, s_recv, pl.ds(0, LAST))
    for d, w, j in CHUNKS:
        gather_from(LAST, d, w, j).wait_recv()
    whole(p_gu, p_dn, a_send, pl.ds(0, LAST))


def place():
    dp = lax.axis_index("dp")
    y, z, c = dp // 8, (dp // 2) % 4, dp % 2
    return dp, z + y * (7 - 2 * z), c


def block_rows(array, d, dev, count=1):
    n = array.shape[1] // 16
    return array.at[d, pl.ds(pl.multiple_of(dev * n, n), n * count)]


def from_chip(q, h, d):
    return (q + CHIPS - h) % CHIPS if d == 0 else (q + h) % CHIPS


def arrived(x, out):
    _, q, _ = place()
    chips = [(d, device_at(from_chip(q, h, d), 0)) for d in range(2) for h in range(LAST)]
    return [(block_rows(x, d, chip, 2), block_rows(out, d, chip, 2)) for d, chip in chips]


def landed(hop, lands, outs):
    _, q, c = place()
    pairs = []
    for i, land in enumerate(lands):
        dev = device_at(from_chip(q, hop, i % 2), c if i < 2 else 1 - c)
        for w, out in enumerate(outs):
            pairs.append((land.at[w] if len(outs) > 1 else land, block_rows(out, i % 2, dev)))
    return pairs


def through(pairs, slots, in_sem, out_sem):
    loads, stores = [], []
    for i, (src, dst) in enumerate(pairs):
        at = slots.at[i % 16, pl.ds(0, src.shape[0])]
        loads.append(pltpu.make_async_copy(src, at, in_sem.at[i % 16]))
        stores.append(pltpu.make_async_copy(at, dst, out_sem.at[i % 16]))
    n = len(pairs)
    for i in range(min(8, n)):
        loads[i].start()
    for i in range(n):
        loads[i].wait()
        stores[i].start()
        if i >= 8:
            stores[i - 8].wait()
        if i + 8 < n:
            loads[i + 8].start()
    for i in range(max(0, n - 8), n):
        stores[i].wait()


def copy_wide(xg, xu, out_g, out_u, slots, in_sem, out_sem):
    through(arrived(xg, out_g) + arrived(xu, out_u), slots, in_sem, out_sem)


def copy_down(*refs):
    factor, x = refs[:2]
    gs, ms, vs = refs[2:5], refs[5:8], refs[8:11]
    out, m_out, v_out = refs[11], refs[12:15], refs[15:18]
    slots, g_gu, g_dn, m_gu, m_dn, v_gu, v_dn, in_sem, out_sem, state_in, state_out = refs[18:]

    def pick(gu, dn, d, w):
        return gu.at[d, w] if w < 2 else dn.at[d]

    def load(d, w):
        i = d * 3 + w
        return [
            pltpu.make_async_copy(gs[w].at[d], pick(g_gu, g_dn, d, w), state_in.at[0, i]),
            pltpu.make_async_copy(ms[w].at[d], pick(m_gu, m_dn, d, w), state_in.at[1, i]),
            pltpu.make_async_copy(vs[w].at[d], pick(v_gu, v_dn, d, w), state_in.at[2, i]),
        ]

    def store(d, w):
        i = d * 3 + w
        return [
            pltpu.make_async_copy(pick(m_gu, m_dn, d, w), m_out[w].at[d], state_out.at[0, i]),
            pltpu.make_async_copy(pick(v_gu, v_dn, d, w), v_out[w].at[d], state_out.at[1, i]),
        ]

    for d, w in BLOCKS:
        for one in load(d, w):
            one.start()
    scale = jnp.broadcast_to(factor[0:1, 0:1], (16, 1024))
    for d, w in BLOCKS:
        for one in load(d, w):
            one.wait()
        gr, mr, vr = pick(g_gu, g_dn, d, w), pick(m_gu, m_dn, d, w), pick(v_gu, v_dn, d, w)

        def update(rows, cols):
            grad = gr[rows, cols].astype(F32) * scale
            mr[rows, cols] = 0.9 * mr[rows, cols] + 0.1 * grad
            vr[rows, cols] = 0.95 * vr[rows, cols] + 0.05 * grad * grad

        tiles(gr, update)
        for one in store(d, w):
            one.start()
    through(arrived(x, out), slots, in_sem, out_sem)
    for d, w in BLOCKS:
        for one in store(d, w):
            one.wait()


def settle(*refs):
    lands, outs, (wide_slots, down_slots, in_sem, out_sem) = refs[3:19], refs[19:22], refs[22:]
    wide = landed(LAST, lands[0:4], outs[:2]) + landed(LAST + 1, lands[4:8], outs[:2])
    down = landed(LAST, lands[8:12], outs[2:]) + landed(LAST + 1, lands[12:16], outs[2:])
    through(wide, wide_slots, in_sem, out_sem)
    through(down, down_slots, in_sem, out_sem)


def finish(weights, *refs):
    lands, outs, sem = refs[weights : weights + 4], refs[weights + 4 : 2 * weights + 4], refs[-1]
    copies = [pltpu.make_async_copy(src, dst, sem.at[i]) for i, (src, dst) in enumerate(landed(LAST + 2, lands, outs))]
    for copy in copies:
        copy.start()
    for copy in copies:
        copy.wait()


def solution(mesh):
    whole = [(2, 1024, 4096), (2, 1024, 4096), (2, 4096, 1024)]
    block = [(2, 64, 4096), (2, 64, 4096), (2, 256, 1024)]

    def shapes(dims, dtype):
        return [jax.ShapeDtypeStruct(s, dtype) for s in dims]

    def pair(lead, dtype):
        return [pltpu.VMEM((*lead, 2, 2, 64, 4096), dtype), pltpu.VMEM((*lead, 2, 256, 1024), dtype)]

    dma = pltpu.SemaphoreType.DMA
    anywhere = pl.BlockSpec(memory_space=pl.ANY)
    hbm = pl.BlockSpec(memory_space=pltpu.HBM)
    vmem = pl.BlockSpec(memory_space=pltpu.VMEM)
    mib = 1024 * 1024

    def local(body, outs, ins, scratch, moved, limit, aliases=None, specs=None):
        return call_local(body, outs, ins, scratch, moved, limit, aliases, specs)

    def call_local(body, outs, ins, scratch, moved, limit, aliases, specs):
        return pl.pallas_call(
            body,
            out_shape=outs,
            in_specs=specs or [hbm] * len(ins),
            out_specs=[hbm] * len(outs),
            scratch_shapes=scratch,
            input_output_aliases=aliases or {},
            cost_estimate=pl.CostEstimate(flops=int(moved * 40), bytes_accessed=int(moved), transcendentals=0),
            compiler_params=pltpu.CompilerParams(vmem_limit_bytes=limit * mib),
        )(*ins)

    def permute(array, pairs):
        return lax.ppermute(array, "dp", pairs)

    def at(q, c):
        return device_at(q % CHIPS, c)

    clockwise = [(at(q, c), at(q + 1, c)) for q in range(CHIPS) for c in range(2)]
    ways = [clockwise, [(b, a) for a, b in clockwise]]
    across = [(i, i ^ 1) for i in range(16)]

    def step(*arrays):
        m, v = arrays[6:9], arrays[9:12]
        out = pl.pallas_call(
            kernel,
            out_shape=[
                *shapes(whole + block, BF16),
                jax.ShapeDtypeStruct((8, 128), F32),
                *shapes([(2, 64, 4096)] * 2 + [(256, 1024)] * 2, BF16),
            ],
            in_specs=[hbm] * 12,
            out_specs=[hbm] * 6 + [vmem] + [hbm] * 4,
            scratch_shapes=[
                *pair((8,), BF16),
                *pair((3,), BF16),
                *pair((2,), BF16),
                *pair((), BF16),
                *pair((), F32),
                *pair((), F32),
                pltpu.VMEM((16, 1024), F32),
                pltpu.VMEM((16, 1, 128), F32),
                dma((2,)), dma((12,)), dma((8, 2)), dma((2,)), dma((3, 12)), dma((2, 2)), dma((3, 2)),
                dma((2,)), dma((2,)), dma((2,)), dma((1,)), dma((1,)), dma((2,)), dma((2,)),
            ],
            compiler_params=pltpu.CompilerParams(collective_id=0, has_side_effects=True, vmem_limit_bytes=66 * 1000 * 1000),
            name="step",
        )(*arrays)
        (xg, xu, xd), sums, factor, (e0, e1, f0, f1) = out[:3], out[3:6], out[6], out[7:]
        slots = [dma((16,)), dma((16,))]

        def hop_on(arrays):
            return [permute(e, ways[d]) for d, e in enumerate(arrays)]

        def cross(arrays):
            return [permute(e, across) for e in arrays]

        wide5, deep5 = [e0, e1], [f0, f1]
        wide6, deep6 = hop_on(wide5), hop_on(deep5)
        their_wide5, their_deep5 = cross(wide5), cross(deep5)
        new_g, new_u = local(
            copy_wide, shapes(whole[:2], BF16), (xg, xu), [pltpu.VMEM((16, 128, 4096), BF16), *slots], 40 * mib, 50
        )
        wide7, their_wide6 = hop_on(wide6), cross(wide6)
        new_d, *state = local(
            copy_down,
            shapes(whole[2:], BF16) + shapes(block * 2, F32),
            (factor, xd, *sums, *m, *v),
            [
                pltpu.VMEM((16, 512, 1024), BF16), *pair((), BF16), *pair((), F32), *pair((), F32),
                *slots, dma((3, 6)), dma((2, 6)),
            ],
            48 * mib,
            50,
            specs=[vmem] + [hbm] * 10,
        )
        deep7, their_deep6 = hop_on(deep6), cross(deep6)
        news = local(
            settle,
            shapes(whole, BF16),
            (new_g, new_u, new_d, *wide5, *their_wide5, *wide6, *their_wide6, *deep5, *their_deep5, *deep6, *their_deep6),
            [pltpu.VMEM((16, 64, 4096), BF16), pltpu.VMEM((16, 256, 1024), BF16), *slots],
            24 * mib,
            24,
            {0: 0, 1: 1, 2: 2},
            [hbm] * 3 + [anywhere] * 16,
        )
        their_wide7 = cross(wide7)
        new_g, new_u = local(
            lambda *refs: finish(2, *refs), shapes(whole[:2], BF16), (*news[:2], *wide7, *their_wide7), [dma((8,))],
            8 * mib, 24, {0: 0, 1: 1}, [hbm] * 2 + [anywhere] * 4,
        )
        their_deep7 = cross(deep7)
        (new_d,) = local(
            lambda *refs: finish(1, *refs), shapes(whole[2:], BF16), (news[2], *deep7, *their_deep7), [dma((8,))],
            4 * mib, 24, {0: 0}, [hbm] + [anywhere] * 4,
        )
        return (new_g, new_u, new_d, *state)

    all_of, cut = P(None, None, None), P(None, "dp", None)
    return jax.shard_map(
        step,
        mesh=mesh,
        in_specs=(P(("rep", "dp"), None, None, None),) * 3 + (all_of,) * 3 + (cut,) * 6,
        out_specs=(P("rep", None, None),) * 3 + (P("rep", "dp", None),) * 6,
        check_vma=False,
    )
```

```python
import jax
import jax.numpy as jnp
from jax import lax
from jax.experimental import pallas as pl
from jax.experimental.pallas import tpu as pltpu
from jax.sharding import PartitionSpec as P


MESH = pl.DeviceIdType.MESH
F32 = jnp.float32
BF16 = jnp.bfloat16
CHIPS = 8
LAST = 5
BLOCKS = [(d, w) for w in range(3) for d in range(2)]
CHUNKS = [(d, w, j) for w in range(3) for j in range(2) for d in range(2)]


def device_at(q, c):
    y = q // 4
    z = q + y * (7 - 2 * q)
    return y * 8 + z * 2 + c


def tiles(ref, body):
    rows, cols = ref.shape

    def strip(r, carry):
        at = pl.ds(pl.multiple_of(r * 16, 16), 16)
        for k in range(cols // 1024):
            body(at, pl.ds(k * 1024, 1024))
        return carry

    lax.fori_loop(0, rows // 16, strip, 0)


def kernel(*refs):
    g, wt, m, v = (refs[i : i + 3] for i in (0, 3, 6, 9))
    x, gsum = refs[12:15], refs[15:18]
    factor_ref = refs[18]
    edge_gu, edge_dn = refs[19:21], refs[21:23]
    (p_gu, p_dn, r_gu, r_dn, o_gu, o_dn, w_gu, w_dn, m_gu, m_dn, v_gu, v_dn, acc, norms) = refs[23:37]
    (p_send, p_recv, r_send, r_recv, o_sem, state_sem, a_send, s_send, s_recv, n_send, n_recv, l_sem, g_sem) = refs[37:]

    rep, dp = lax.axis_index("rep"), lax.axis_index("dp")
    y, z, c = dp // 8, (dp // 2) % 4, dp % 2
    q = z + y * (7 - 2 * z)
    nxt = [(rep, device_at((q + 1) % CHIPS, c)), (rep, device_at((q + 7) % CHIPS, c))]
    partner = (rep, dp + 1 - 2 * c)

    def half(w, j, start=0):
        n = 32 if w < 2 else 128
        if j is None:
            return pl.ds(start, 2 * n)
        return pl.ds(start + j * n, n)

    def pick(gu, dn, lead, d, w, j=None):
        return gu.at[(*lead, d, w, half(w, j))] if w < 2 else dn.at[(*lead, d, half(w, j))]

    def rows_of(array, w, d, dev, lead=(), j=None):
        n = 64 if w < 2 else 256
        return array[w].at[(*lead, d, half(w, j, pl.multiple_of(dev * n, n)), slice(None))]

    def flag(d, w, j):
        return (d * 3 + w) * 2 + j

    def scattered(s, d):
        return (q + 7 - s + CHIPS) % CHIPS if d == 0 else (q + 1 + s) % CHIPS

    def gathered(h, d):
        return (q + CHIPS - h) % CHIPS if d == 0 else (q + h) % CHIPS

    def whole(gu, dn, sem, *lead):
        for i, part in enumerate((gu, dn)):
            ref = part.at[lead] if lead else part
            pltpu.make_async_copy(ref, ref, sem.at[i]).wait()

    def own_load(s, d, w):
        return pltpu.make_async_copy(
            rows_of(g, w, d, device_at(scattered(s, d), c), (0,)), pick(o_gu, o_dn, (s % 2,), d, w), o_sem.at[s % 2, w // 2]
        )

    def to_partner(s, d, w, j):
        return pltpu.make_async_remote_copy(
            rows_of(g, w, d, device_at(scattered(s, d), 1 - c), (0,), j),
            pick(p_gu, p_dn, (s,), d, w, j),
            p_send.at[w // 2],
            r_recv.at[2, flag(d, w, j)] if isinstance(s, int) and s == 0 else p_recv.at[s, w // 2],
            device_id=partner,
            device_id_type=MESH,
        )

    def hop(s, d, w, j):
        return pltpu.make_async_remote_copy(
            pick(p_gu, p_dn, (s,), d, w, j),
            pick(r_gu, r_dn, (s % 3,), d, w, j),
            r_send.at[w // 2],
            r_recv.at[s % 3, flag(d, w, j)],
            device_id=nxt[d],
            device_id_type=MESH,
        )

    def state_loads(d, w):
        return [
            pltpu.make_async_copy(m[w].at[d], pick(m_gu, m_dn, (), d, w), state_sem.at[0, w // 2]),
            pltpu.make_async_copy(v[w].at[d], pick(v_gu, v_dn, (), d, w), state_sem.at[1, w // 2]),
            pltpu.make_async_copy(rows_of(wt, w, d, dp), pick(w_gu, w_dn, (), d, w), state_sem.at[2, w // 2]),
        ]

    def sum_out(d, w):
        return pltpu.make_async_copy(pick(p_gu, p_dn, (7,), d, w), gsum[w].at[d], g_sem.at[w // 2])

    barrier = pltpu.get_barrier_semaphore()
    for dev in (*nxt, partner):
        pl.semaphore_signal(barrier, inc=1, device_id=dev, device_id_type=MESH)
    for d, w in BLOCKS:
        own_load(0, d, w).start()
    pl.semaphore_wait(barrier, 3)
    for s in (0, 1):
        for d, w, j in CHUNKS:
            to_partner(s, d, w, j).start()

    def scatter_step(s, first, last):
        if not last:
            for d, w in BLOCKS:
                own_load(s + 1, d, w).start()
            if first:
                for d, w, j in CHUNKS:
                    to_partner(s + 2, d, w, j).start()
            else:

                @pl.when(s < 6)
                def _():
                    for d, w, j in CHUNKS:
                        to_partner(s + 2, d, w, j).start()

        whole(o_gu, o_dn, o_sem.at[s % 2], s % 2)
        if not first:
            whole(p_gu, p_dn, p_recv.at[s], s)
        for d, w, j in CHUNKS:
            own, theirs = pick(o_gu, o_dn, (s % 2,), d, w, j), pick(p_gu, p_dn, (s,), d, w, j)
            if first:
                to_partner(s, d, w, j).wait_recv()

                def add(rows, cols):
                    theirs[rows, cols] = (own[rows, cols].astype(F32) + theirs[rows, cols].astype(F32)).astype(BF16)

            else:
                before = (s + 2) % 3
                so_far = pick(r_gu, r_dn, (before,), d, w, j)
                hop(s - 1, d, w, j).wait_recv()

                def add(rows, cols):
                    total = (own[rows, cols].astype(F32) + theirs[rows, cols].astype(F32)) + so_far[rows, cols].astype(F32)
                    total = total.astype(BF16)
                    theirs[rows, cols] = total
                    if last:
                        acc[...] += total.astype(F32) * total.astype(F32)

            tiles(theirs, add)
            if last:
                if j == 1:
                    sum_out(d, w).start()
            else:
                hop(s, d, w, j).start()

    scatter_step(0, True, False)
    for d, w in BLOCKS:
        for copy in state_loads(d, w):
            copy.start()
    acc[...] = jnp.zeros_like(acc)
    lax.fori_loop(1, 7, lambda s, carry: (scatter_step(s, False, False), carry)[1], 0)
    scatter_step(7, False, True)

    mine = acc[0:8, 0:128] + acc[8:16, 0:128]
    for k in range(1, 8):
        at = pl.ds(k * 128, 128)
        mine += acc[0:8, at] + acc[8:16, at]
    norms[dp] = jnp.sum(mine, axis=0, keepdims=True)
    for r in range(1, 16):
        pltpu.make_async_remote_copy(
            norms.at[dp], norms.at[dp], n_send.at[0], n_recv.at[0], device_id=(rep, (dp + r) % 16), device_id_type=MESH
        ).start()
    whole(p_gu, p_dn, r_send, pl.ds(0, 7))
    whole(p_gu, p_dn, p_send)
    for i, (gu, dn) in enumerate(((m_gu, m_dn), (v_gu, v_dn), (w_gu, w_dn))):
        whole(gu, dn, state_sem.at[i])
    others = norms.at[pl.ds(0, 15)]
    pltpu.make_async_copy(others, others, n_send.at[0]).wait()
    pltpu.make_async_copy(others, others, n_recv.at[0]).wait()
    squares = norms[0]
    for k in range(1, 16):
        squares += norms[k]
    count = 16 * 2 * (64 * 4096 * 2 + 256 * 1024)
    mean = jnp.sum(squares) * (1.0 / count)
    factor = jnp.minimum(1.0, 0.5 * lax.rsqrt(jnp.full((8, 128), mean, F32) + 1e-30))
    factor_ref[...] = factor
    scale = jnp.broadcast_to(factor[0:1, 0:1], (16, 1024))

    def edge(d, w, j):
        return edge_gu[d].at[w, half(w, j)] if w < 2 else edge_dn[d].at[half(w, j)]

    def held(h, d, w, j):
        if isinstance(h, int) and h == 0:
            return pick(p_gu, p_dn, (0,), d, w, j)
        if isinstance(h, int) and h == LAST:
            return edge(d, w, j)
        return rows_of(x, w, d, device_at(gathered(h, d), c), (), j)

    def gather_hop(h, d, w, j):
        dst = edge(d, w, j) if isinstance(h, int) and h == LAST - 1 else rows_of(x, w, d, device_at(gathered(h, d), c), (), j)
        return pltpu.make_async_remote_copy(
            held(h, d, w, j), dst, a_send.at[w // 2], r_recv.at[(h + 1) % 3, flag(d, w, j)], device_id=nxt[d], device_id_type=MESH
        )

    def gather_from(h, d, w, j):
        block = held(h, d, w, j)
        return pltpu.make_async_remote_copy(
            block, block, a_send.at[w // 2], r_recv.at[h % 3, flag(d, w, j)], device_id=nxt[d], device_id_type=MESH
        )

    def share(h, d, w, j):
        return pltpu.make_async_remote_copy(
            held(h, d, w, j),
            rows_of(x, w, d, device_at(gathered(h, d), c), (), j),
            s_send.at[w // 2],
            s_recv.at[w // 2],
            device_id=partner,
            device_id_type=MESH,
        )

    def keep(d, w):
        return pltpu.make_async_copy(pick(p_gu, p_dn, (0,), d, w), rows_of(x, w, d, dp), l_sem.at[w // 2])

    for d, w, j in CHUNKS:
        gr, new = pick(p_gu, p_dn, (7,), d, w, j), pick(p_gu, p_dn, (0,), d, w, j)
        mr, vr, wr = pick(m_gu, m_dn, (), d, w, j), pick(v_gu, v_dn, (), d, w, j), pick(w_gu, w_dn, (), d, w, j)

        def update(rows, cols):
            grad = gr[rows, cols].astype(F32) * scale
            m1 = 0.9 * mr[rows, cols] + 0.1 * grad
            v1 = 0.95 * vr[rows, cols] + 0.05 * grad * grad
            old = wr[rows, cols].astype(F32)
            new[rows, cols] = (old - 0.02 * (m1 * lax.rsqrt(v1 + 1e-8) + 0.1 * old)).astype(BF16)

        tiles(new, update)
        gather_hop(0, d, w, j).start()
        share(0, d, w, j).start()
        if j == 1:
            keep(d, w).start()

    def gather_step(h, carry):
        for d, w, j in CHUNKS:
            gather_from(h, d, w, j).wait_recv()
            gather_hop(h, d, w, j).start()
            share(h, d, w, j).start()
        return carry

    lax.fori_loop(1, LAST - 1, gather_step, 0)
    gather_step(LAST - 1, 0)
    whole(p_gu, p_dn, l_sem, 0)
    whole(p_gu, p_dn, g_sem, 7)
    whole(p_gu, p_dn, s_send, pl.ds(0, LAST))
    whole(p_gu, p_dn, s_recv, pl.ds(0, LAST))
    for d, w, j in CHUNKS:
        gather_from(LAST, d, w, j).wait_recv()
    whole(p_gu, p_dn, a_send, pl.ds(0, LAST))


def place():
    dp = lax.axis_index("dp")
    y, z, c = dp // 8, (dp // 2) % 4, dp % 2
    return dp, z + y * (7 - 2 * z), c


def block_rows(array, d, dev, count=1):
    n = array.shape[1] // 16
    return array.at[d, pl.ds(pl.multiple_of(dev * n, n), n * count)]


def from_chip(q, h, d):
    return (q + CHIPS - h) % CHIPS if d == 0 else (q + h) % CHIPS


def arrived(x, out):
    _, q, _ = place()
    chips = [(d, device_at(from_chip(q, h, d), 0)) for d in range(2) for h in range(LAST)]
    return [(block_rows(x, d, chip, 2), block_rows(out, d, chip, 2)) for d, chip in chips]


def landed(hop, lands, outs, first=0, at=None):
    _, q, c = place()
    pairs = []
    for i, land in enumerate(lands, first):
        dev = device_at(from_chip(q, hop, i % 2), c if i < 2 else 1 - c)
        for w, out in enumerate(outs):
            target = block_rows(out, i % 2, dev)
            pairs.append((land.at[w] if len(outs) > 1 else land, target if at is None else target.at[at]))
    return pairs


def through(pairs, slots, in_sem, out_sem):
    loads, stores = [], []
    for i, (src, dst) in enumerate(pairs):
        at = slots.at[i % 16, pl.ds(0, src.shape[0])]
        loads.append(pltpu.make_async_copy(src, at, in_sem.at[i % 16]))
        stores.append(pltpu.make_async_copy(at, dst, out_sem.at[i % 16]))
    n = len(pairs)
    for i in range(min(8, n)):
        loads[i].start()
    for i in range(n):
        loads[i].wait()
        stores[i].start()
        if i >= 8:
            stores[i - 8].wait()
        if i + 8 < n:
            loads[i + 8].start()
    for i in range(max(0, n - 8), n):
        stores[i].wait()


def copy_wide(xg, xu, out_g, out_u, slots, in_sem, out_sem):
    through(arrived(xg, out_g) + arrived(xu, out_u), slots, in_sem, out_sem)


def copy_down(*refs):
    factor, x = refs[:2]
    gs, ms, vs = refs[2:5], refs[5:8], refs[8:11]
    out, m_out, v_out = refs[11], refs[12:15], refs[15:18]
    slots, g_gu, g_dn, m_gu, m_dn, v_gu, v_dn, in_sem, out_sem, state_in, state_out = refs[18:]

    def pick(gu, dn, d, w):
        return gu.at[d, w] if w < 2 else dn.at[d]

    def load(d, w):
        i = d * 3 + w
        return [
            pltpu.make_async_copy(gs[w].at[d], pick(g_gu, g_dn, d, w), state_in.at[0, i]),
            pltpu.make_async_copy(ms[w].at[d], pick(m_gu, m_dn, d, w), state_in.at[1, i]),
            pltpu.make_async_copy(vs[w].at[d], pick(v_gu, v_dn, d, w), state_in.at[2, i]),
        ]

    def store(d, w):
        i = d * 3 + w
        return [
            pltpu.make_async_copy(pick(m_gu, m_dn, d, w), m_out[w].at[d], state_out.at[0, i]),
            pltpu.make_async_copy(pick(v_gu, v_dn, d, w), v_out[w].at[d], state_out.at[1, i]),
        ]

    for d, w in BLOCKS:
        for one in load(d, w):
            one.start()
    scale = jnp.broadcast_to(factor[0:1, 0:1], (16, 1024))
    for d, w in BLOCKS:
        for one in load(d, w):
            one.wait()
        gr, mr, vr = pick(g_gu, g_dn, d, w), pick(m_gu, m_dn, d, w), pick(v_gu, v_dn, d, w)

        def update(rows, cols):
            grad = gr[rows, cols].astype(F32) * scale
            mr[rows, cols] = 0.9 * mr[rows, cols] + 0.1 * grad
            vr[rows, cols] = 0.95 * vr[rows, cols] + 0.05 * grad * grad

        tiles(gr, update)
        for one in store(d, w):
            one.start()
    through(arrived(x, out), slots, in_sem, out_sem)
    for d, w in BLOCKS:
        for one in store(d, w):
            one.wait()


def settle(*refs):
    lands, outs, (wide_slots, down_slots, in_sem, out_sem) = refs[3:19], refs[19:22], refs[22:]
    wide = landed(LAST, lands[0:4], outs[:2]) + landed(LAST + 1, lands[4:8], outs[:2])
    down = landed(LAST, lands[8:12], outs[2:]) + landed(LAST + 1, lands[12:16], outs[2:])
    through(wide, wide_slots, in_sem, out_sem)
    through(down, down_slots, in_sem, out_sem)


def in_place(pairs, sem):
    copies = [pltpu.make_async_copy(src, dst, sem.at[i]) for i, (src, dst) in enumerate(pairs)]
    for copy in copies:
        copy.start()
    for copy in copies:
        copy.wait()


def finish_wide(*refs):
    through(landed(LAST + 2, refs[2:6], refs[6:8]), *refs[8:])


def finish_deep(*refs):
    in_place(landed(LAST + 2, refs[1:5], refs[5:6], 0, pl.ds(0, 128)), refs[6])


def finish_tail(*refs):
    in_place(landed(LAST + 2, refs[1:5], refs[5:6], 0, pl.ds(128, 128)), refs[6])


def solution(mesh):
    whole = [(2, 1024, 4096), (2, 1024, 4096), (2, 4096, 1024)]
    block = [(2, 64, 4096), (2, 64, 4096), (2, 256, 1024)]

    def shapes(dims, dtype):
        return [jax.ShapeDtypeStruct(s, dtype) for s in dims]

    def pair(lead, dtype):
        return [pltpu.VMEM((*lead, 2, 2, 64, 4096), dtype), pltpu.VMEM((*lead, 2, 256, 1024), dtype)]

    dma = pltpu.SemaphoreType.DMA
    anywhere = pl.BlockSpec(memory_space=pl.ANY)
    hbm = pl.BlockSpec(memory_space=pltpu.HBM)
    vmem = pl.BlockSpec(memory_space=pltpu.VMEM)
    mib = 1024 * 1024

    def local(body, outs, ins, scratch, moved, limit, aliases=None, specs=None):
        return call_local(body, outs, ins, scratch, moved, limit, aliases, specs)

    def call_local(body, outs, ins, scratch, moved, limit, aliases, specs):
        return pl.pallas_call(
            body,
            out_shape=outs,
            in_specs=specs or [hbm] * len(ins),
            out_specs=[hbm] * len(outs),
            scratch_shapes=scratch,
            input_output_aliases=aliases or {},
            cost_estimate=pl.CostEstimate(flops=int(moved * 40), bytes_accessed=int(moved), transcendentals=0),
            compiler_params=pltpu.CompilerParams(vmem_limit_bytes=limit * mib),
        )(*ins)

    def permute(array, pairs):
        return lax.ppermute(array, "dp", pairs)

    def at(q, c):
        return device_at(q % CHIPS, c)

    clockwise = [(at(q, c), at(q + 1, c)) for q in range(CHIPS) for c in range(2)]
    ways = [clockwise, [(b, a) for a, b in clockwise]]
    across = [(i, i ^ 1) for i in range(16)]

    def step(*arrays):
        m, v = arrays[6:9], arrays[9:12]
        out = pl.pallas_call(
            kernel,
            out_shape=[
                *shapes(whole + block, BF16),
                jax.ShapeDtypeStruct((8, 128), F32),
                *shapes([(2, 64, 4096)] * 2 + [(256, 1024)] * 2, BF16),
            ],
            in_specs=[hbm] * 12,
            out_specs=[hbm] * 6 + [vmem] + [hbm] * 4,
            scratch_shapes=[
                *pair((8,), BF16),
                *pair((3,), BF16),
                *pair((2,), BF16),
                *pair((), BF16),
                *pair((), F32),
                *pair((), F32),
                pltpu.VMEM((16, 1024), F32),
                pltpu.VMEM((16, 1, 128), F32),
                dma((2,)), dma((8, 2)), dma((2,)), dma((3, 12)), dma((2, 2)), dma((3, 2)),
                dma((2,)), dma((2,)), dma((2,)), dma((1,)), dma((1,)), dma((2,)), dma((2,)),
            ],
            compiler_params=pltpu.CompilerParams(collective_id=0, has_side_effects=True, vmem_limit_bytes=66 * 1000 * 1000),
            name="step",
        )(*arrays)
        (xg, xu, xd), sums, factor, (e0, e1, f0, f1) = out[:3], out[3:6], out[6], out[7:]
        slots = [dma((16,)), dma((16,))]

        def hop_on(arrays):
            return [permute(e, ways[d]) for d, e in enumerate(arrays)]

        def cross(arrays):
            return [permute(e, across) for e in arrays]

        wide5, deep5 = [e0, e1], [f0, f1]
        wide6, deep6 = hop_on(wide5), hop_on(deep5)
        their_wide5, their_deep5 = cross(wide5), cross(deep5)
        new_g, new_u = local(
            copy_wide, shapes(whole[:2], BF16), (xg, xu), [pltpu.VMEM((16, 128, 4096), BF16), *slots], 40 * mib, 50
        )
        wide7, their_wide6 = hop_on(wide6), cross(wide6)
        new_d, *state = local(
            copy_down,
            shapes(whole[2:], BF16) + shapes(block * 2, F32),
            (factor, xd, *sums, *m, *v),
            [
                pltpu.VMEM((16, 512, 1024), BF16), *pair((), BF16), *pair((), F32), *pair((), F32),
                *slots, dma((3, 6)), dma((2, 6)),
            ],
            48 * mib,
            50,
            specs=[vmem] + [hbm] * 10,
        )
        deep7, their_deep6 = hop_on([e[:128] for e in deep6]), cross(deep6)
        tail7 = hop_on([e[128:] for e in deep6])
        news = local(
            settle,
            shapes(whole, BF16),
            (new_g, new_u, new_d, *wide5, *their_wide5, *wide6, *their_wide6, *deep5, *their_deep5, *deep6, *their_deep6),
            [pltpu.VMEM((16, 64, 4096), BF16), pltpu.VMEM((16, 256, 1024), BF16), *slots],
            24 * mib,
            24,
            {0: 0, 1: 1, 2: 2},
            [hbm] * 3 + [anywhere] * 16,
        )
        their_wide7 = cross(wide7)
        new_g, new_u = local(
            finish_wide, shapes(whole[:2], BF16), (*news[:2], *wide7, *their_wide7),
            [pltpu.VMEM((16, 64, 4096), BF16), *slots],
            8 * mib, 24, {0: 0, 1: 1}, [hbm] * 2 + [anywhere] * 4,
        )
        their_deep7 = cross(deep7)
        their_tail7 = cross(tail7)
        (new_d,) = local(
            finish_deep, shapes(whole[2:], BF16), (news[2], *deep7, *their_deep7), [dma((4,))],
            2 * mib, 24, {0: 0}, [hbm] + [anywhere] * 4,
        )
        (new_d,) = local(
            finish_tail, shapes(whole[2:], BF16), (new_d, *tail7, *their_tail7), [dma((4,))], 2 * mib, 24,
            {0: 0}, [hbm] + [anywhere] * 4,
        )
        return (new_g, new_u, new_d, *state)

    all_of, cut = P(None, None, None), P(None, "dp", None)
    return jax.shard_map(
        step,
        mesh=mesh,
        in_specs=(P(("rep", "dp"), None, None, None),) * 3 + (all_of,) * 3 + (cut,) * 6,
        out_specs=(P("rep", None, None),) * 3 + (P("rep", "dp", None),) * 6,
        check_vma=False,
    )
```

```python
import jax
import jax.numpy as jnp
from jax import lax
from jax.experimental import pallas as pl
from jax.experimental.pallas import tpu as pltpu
from jax.sharding import PartitionSpec as P


MESH = pl.DeviceIdType.MESH
F32 = jnp.float32
BF16 = jnp.bfloat16
CHIPS = 8
LAST = 5
BLOCKS = [(d, w) for w in range(3) for d in range(2)]
CHUNKS = [(d, w, j) for w in range(3) for j in range(2) for d in range(2)]


def device_at(q, c):
    y = q // 4
    z = q + y * (7 - 2 * q)
    return y * 8 + z * 2 + c


def tiles(ref, body):
    rows, cols = ref.shape

    def strip(r, carry):
        at = pl.ds(pl.multiple_of(r * 16, 16), 16)
        for k in range(cols // 1024):
            body(at, pl.ds(k * 1024, 1024))
        return carry

    lax.fori_loop(0, rows // 16, strip, 0)


def kernel(*refs):
    g, wt, m, v = (refs[i : i + 3] for i in (0, 3, 6, 9))
    x, gsum = refs[12:15], refs[15:18]
    factor_ref = refs[18]
    edge_gu, edge_dn = refs[19:21], refs[21:23]
    (p_gu, p_dn, r_gu, r_dn, o_gu, o_dn, w_gu, w_dn, m_gu, m_dn, v_gu, v_dn, acc, norms) = refs[23:37]
    (p_send, p_recv, r_send, r_recv, o_sem, state_sem, a_send, s_send, s_recv, n_send, n_recv, l_sem, g_sem) = refs[37:]

    rep, dp = lax.axis_index("rep"), lax.axis_index("dp")
    y, z, c = dp // 8, (dp // 2) % 4, dp % 2
    q = z + y * (7 - 2 * z)
    nxt = [(rep, device_at((q + 1) % CHIPS, c)), (rep, device_at((q + 7) % CHIPS, c))]
    partner = (rep, dp + 1 - 2 * c)

    def half(w, j, start=0):
        n = 32 if w < 2 else 128
        if j is None:
            return pl.ds(start, 2 * n)
        return pl.ds(start + j * n, n)

    def pick(gu, dn, lead, d, w, j=None):
        return gu.at[(*lead, d, w, half(w, j))] if w < 2 else dn.at[(*lead, d, half(w, j))]

    def rows_of(array, w, d, dev, lead=(), j=None):
        n = 64 if w < 2 else 256
        return array[w].at[(*lead, d, half(w, j, pl.multiple_of(dev * n, n)), slice(None))]

    def flag(d, w, j):
        return (d * 3 + w) * 2 + j

    def scattered(s, d):
        return (q + 7 - s + CHIPS) % CHIPS if d == 0 else (q + 1 + s) % CHIPS

    def gathered(h, d):
        return (q + CHIPS - h) % CHIPS if d == 0 else (q + h) % CHIPS

    def whole(gu, dn, sem, *lead):
        for i, part in enumerate((gu, dn)):
            ref = part.at[lead] if lead else part
            pltpu.make_async_copy(ref, ref, sem.at[i]).wait()

    def own_load(s, d, w):
        return pltpu.make_async_copy(
            rows_of(g, w, d, device_at(scattered(s, d), c), (0,)), pick(o_gu, o_dn, (s % 2,), d, w), o_sem.at[s % 2, w // 2]
        )

    def to_partner(s, d, w, j):
        return pltpu.make_async_remote_copy(
            rows_of(g, w, d, device_at(scattered(s, d), 1 - c), (0,), j),
            pick(p_gu, p_dn, (s,), d, w, j),
            p_send.at[w // 2],
            r_recv.at[2, flag(d, w, j)] if isinstance(s, int) and s == 0 else p_recv.at[s, w // 2],
            device_id=partner,
            device_id_type=MESH,
        )

    def hop(s, d, w, j):
        return pltpu.make_async_remote_copy(
            pick(p_gu, p_dn, (s,), d, w, j),
            pick(r_gu, r_dn, (s % 3,), d, w, j),
            r_send.at[w // 2],
            r_recv.at[s % 3, flag(d, w, j)],
            device_id=nxt[d],
            device_id_type=MESH,
        )

    def state_loads(d, w):
        return [
            pltpu.make_async_copy(m[w].at[d], pick(m_gu, m_dn, (), d, w), state_sem.at[0, w // 2]),
            pltpu.make_async_copy(v[w].at[d], pick(v_gu, v_dn, (), d, w), state_sem.at[1, w // 2]),
            pltpu.make_async_copy(rows_of(wt, w, d, dp), pick(w_gu, w_dn, (), d, w), state_sem.at[2, w // 2]),
        ]

    def sum_out(d, w):
        return pltpu.make_async_copy(pick(p_gu, p_dn, (7,), d, w), gsum[w].at[d], g_sem.at[w // 2])

    barrier = pltpu.get_barrier_semaphore()
    for dev in (*nxt, partner):
        pl.semaphore_signal(barrier, inc=1, device_id=dev, device_id_type=MESH)
    for d, w in BLOCKS:
        own_load(0, d, w).start()
    pl.semaphore_wait(barrier, 3)
    for s in (0, 1):
        for d, w, j in CHUNKS:
            to_partner(s, d, w, j).start()

    def scatter_step(s, first, last):
        if not last:
            for d, w in BLOCKS:
                own_load(s + 1, d, w).start()
            if first:
                for d, w, j in CHUNKS:
                    to_partner(s + 2, d, w, j).start()
            else:

                @pl.when(s < 6)
                def _():
                    for d, w, j in CHUNKS:
                        to_partner(s + 2, d, w, j).start()

        whole(o_gu, o_dn, o_sem.at[s % 2], s % 2)
        if not first:
            whole(p_gu, p_dn, p_recv.at[s], s)
        for d, w, j in CHUNKS:
            own, theirs = pick(o_gu, o_dn, (s % 2,), d, w, j), pick(p_gu, p_dn, (s,), d, w, j)
            if first:
                to_partner(s, d, w, j).wait_recv()

                def add(rows, cols):
                    theirs[rows, cols] = (own[rows, cols].astype(F32) + theirs[rows, cols].astype(F32)).astype(BF16)

            else:
                before = (s + 2) % 3
                so_far = pick(r_gu, r_dn, (before,), d, w, j)
                hop(s - 1, d, w, j).wait_recv()

                def add(rows, cols):
                    total = (own[rows, cols].astype(F32) + theirs[rows, cols].astype(F32)) + so_far[rows, cols].astype(F32)
                    total = total.astype(BF16)
                    theirs[rows, cols] = total
                    if last:
                        acc[...] += total.astype(F32) * total.astype(F32)

            tiles(theirs, add)
            if last:
                if j == 1:
                    sum_out(d, w).start()
            else:
                hop(s, d, w, j).start()

    scatter_step(0, True, False)
    for d, w in BLOCKS:
        for copy in state_loads(d, w):
            copy.start()
    acc[...] = jnp.zeros_like(acc)
    lax.fori_loop(1, 7, lambda s, carry: (scatter_step(s, False, False), carry)[1], 0)
    scatter_step(7, False, True)

    mine = acc[0:8, 0:128] + acc[8:16, 0:128]
    for k in range(1, 8):
        at = pl.ds(k * 128, 128)
        mine += acc[0:8, at] + acc[8:16, at]
    norms[dp] = jnp.sum(mine, axis=0, keepdims=True)
    for r in range(1, 16):
        pltpu.make_async_remote_copy(
            norms.at[dp], norms.at[dp], n_send.at[0], n_recv.at[0], device_id=(rep, (dp + r) % 16), device_id_type=MESH
        ).start()
    whole(p_gu, p_dn, r_send, pl.ds(0, 7))
    whole(p_gu, p_dn, p_send)
    for i, (gu, dn) in enumerate(((m_gu, m_dn), (v_gu, v_dn), (w_gu, w_dn))):
        whole(gu, dn, state_sem.at[i])
    others = norms.at[pl.ds(0, 15)]
    pltpu.make_async_copy(others, others, n_send.at[0]).wait()
    pltpu.make_async_copy(others, others, n_recv.at[0]).wait()
    squares = norms[0]
    for k in range(1, 16):
        squares += norms[k]
    count = 16 * 2 * (64 * 4096 * 2 + 256 * 1024)
    mean = jnp.sum(squares) * (1.0 / count)
    factor = jnp.minimum(1.0, 0.5 * lax.rsqrt(jnp.full((8, 128), mean, F32) + 1e-30))
    factor_ref[...] = factor
    scale = jnp.broadcast_to(factor[0:1, 0:1], (16, 1024))

    def edge(d, w, j):
        return edge_gu[d].at[w, half(w, j)] if w < 2 else edge_dn[d].at[half(w, j)]

    def held(h, d, w, j):
        if isinstance(h, int) and h == 0:
            return pick(p_gu, p_dn, (0,), d, w, j)
        if isinstance(h, int) and h == LAST:
            return edge(d, w, j)
        return rows_of(x, w, d, device_at(gathered(h, d), c), (), j)

    def gather_hop(h, d, w, j):
        dst = edge(d, w, j) if isinstance(h, int) and h == LAST - 1 else rows_of(x, w, d, device_at(gathered(h, d), c), (), j)
        return pltpu.make_async_remote_copy(
            held(h, d, w, j), dst, a_send.at[w // 2], r_recv.at[(h + 1) % 3, flag(d, w, j)], device_id=nxt[d], device_id_type=MESH
        )

    def gather_from(h, d, w, j):
        block = held(h, d, w, j)
        return pltpu.make_async_remote_copy(
            block, block, a_send.at[w // 2], r_recv.at[h % 3, flag(d, w, j)], device_id=nxt[d], device_id_type=MESH
        )

    def share(h, d, w, j):
        return pltpu.make_async_remote_copy(
            held(h, d, w, j),
            rows_of(x, w, d, device_at(gathered(h, d), c), (), j),
            s_send.at[w // 2],
            s_recv.at[w // 2],
            device_id=partner,
            device_id_type=MESH,
        )

    def keep(d, w):
        return pltpu.make_async_copy(pick(p_gu, p_dn, (0,), d, w), rows_of(x, w, d, dp), l_sem.at[w // 2])

    for d, w, j in CHUNKS:
        gr, new = pick(p_gu, p_dn, (7,), d, w, j), pick(p_gu, p_dn, (0,), d, w, j)
        mr, vr, wr = pick(m_gu, m_dn, (), d, w, j), pick(v_gu, v_dn, (), d, w, j), pick(w_gu, w_dn, (), d, w, j)

        def update(rows, cols):
            grad = gr[rows, cols].astype(F32) * scale
            m1 = 0.9 * mr[rows, cols] + 0.1 * grad
            v1 = 0.95 * vr[rows, cols] + 0.05 * grad * grad
            old = wr[rows, cols].astype(F32)
            new[rows, cols] = (old - 0.02 * (m1 * lax.rsqrt(v1 + 1e-8) + 0.1 * old)).astype(BF16)

        tiles(new, update)
        gather_hop(0, d, w, j).start()
        share(0, d, w, j).start()
        if j == 1:
            keep(d, w).start()

    def gather_step(h, carry):
        for d, w, j in CHUNKS:
            gather_from(h, d, w, j).wait_recv()
            gather_hop(h, d, w, j).start()
            share(h, d, w, j).start()
        return carry

    lax.fori_loop(1, LAST - 1, gather_step, 0)
    gather_step(LAST - 1, 0)
    whole(p_gu, p_dn, l_sem, 0)
    whole(p_gu, p_dn, g_sem, 7)
    whole(p_gu, p_dn, s_send, pl.ds(0, LAST))
    whole(p_gu, p_dn, s_recv, pl.ds(0, LAST))
    for d, w, j in CHUNKS:
        gather_from(LAST, d, w, j).wait_recv()
    whole(p_gu, p_dn, a_send, pl.ds(0, LAST))


def place():
    dp = lax.axis_index("dp")
    y, z, c = dp // 8, (dp // 2) % 4, dp % 2
    return dp, z + y * (7 - 2 * z), c


def block_rows(array, d, dev, count=1):
    n = array.shape[1] // 16
    return array.at[d, pl.ds(pl.multiple_of(dev * n, n), n * count)]


def from_chip(q, h, d):
    return (q + CHIPS - h) % CHIPS if d == 0 else (q + h) % CHIPS


def arrived(x, out):
    _, q, _ = place()
    chips = [(d, device_at(from_chip(q, h, d), 0)) for d in range(2) for h in range(LAST)]
    return [(block_rows(x, d, chip, 2), block_rows(out, d, chip, 2)) for d, chip in chips]


def landed(hop, lands, outs, first=0, at=None):
    _, q, c = place()
    pairs = []
    for i, land in enumerate(lands, first):
        dev = device_at(from_chip(q, hop, i % 2), c if i < 2 else 1 - c)
        for w, out in enumerate(outs):
            target = block_rows(out, i % 2, dev)
            pairs.append((land.at[w] if len(outs) > 1 else land, target if at is None else target.at[at]))
    return pairs


def through(pairs, slots, in_sem, out_sem):
    loads, stores = [], []
    for i, (src, dst) in enumerate(pairs):
        at = slots.at[i % 16, pl.ds(0, src.shape[0])]
        loads.append(pltpu.make_async_copy(src, at, in_sem.at[i % 16]))
        stores.append(pltpu.make_async_copy(at, dst, out_sem.at[i % 16]))
    n = len(pairs)
    for i in range(min(8, n)):
        loads[i].start()
    for i in range(n):
        loads[i].wait()
        stores[i].start()
        if i >= 8:
            stores[i - 8].wait()
        if i + 8 < n:
            loads[i + 8].start()
    for i in range(max(0, n - 8), n):
        stores[i].wait()


def copy_wide(xg, xu, out_g, out_u, slots, in_sem, out_sem):
    through(arrived(xg, out_g) + arrived(xu, out_u), slots, in_sem, out_sem)


def copy_down(*refs):
    factor, x = refs[:2]
    gs, ms, vs = refs[2:5], refs[5:8], refs[8:11]
    out, m_out, v_out = refs[11], refs[12:15], refs[15:18]
    slots, g_gu, g_dn, m_gu, m_dn, v_gu, v_dn, in_sem, out_sem, state_in, state_out = refs[18:]

    def pick(gu, dn, d, w):
        return gu.at[d, w] if w < 2 else dn.at[d]

    def load(d, w):
        i = d * 3 + w
        return [
            pltpu.make_async_copy(gs[w].at[d], pick(g_gu, g_dn, d, w), state_in.at[0, i]),
            pltpu.make_async_copy(ms[w].at[d], pick(m_gu, m_dn, d, w), state_in.at[1, i]),
            pltpu.make_async_copy(vs[w].at[d], pick(v_gu, v_dn, d, w), state_in.at[2, i]),
        ]

    def store(d, w):
        i = d * 3 + w
        return [
            pltpu.make_async_copy(pick(m_gu, m_dn, d, w), m_out[w].at[d], state_out.at[0, i]),
            pltpu.make_async_copy(pick(v_gu, v_dn, d, w), v_out[w].at[d], state_out.at[1, i]),
        ]

    for d, w in BLOCKS:
        for one in load(d, w):
            one.start()
    scale = jnp.broadcast_to(factor[0:1, 0:1], (16, 1024))
    for d, w in BLOCKS:
        for one in load(d, w):
            one.wait()
        gr, mr, vr = pick(g_gu, g_dn, d, w), pick(m_gu, m_dn, d, w), pick(v_gu, v_dn, d, w)

        def update(rows, cols):
            grad = gr[rows, cols].astype(F32) * scale
            mr[rows, cols] = 0.9 * mr[rows, cols] + 0.1 * grad
            vr[rows, cols] = 0.95 * vr[rows, cols] + 0.05 * grad * grad

        tiles(gr, update)
        for one in store(d, w):
            one.start()
    through(arrived(x, out), slots, in_sem, out_sem)
    for d, w in BLOCKS:
        for one in store(d, w):
            one.wait()


def settle(*refs):
    lands, outs, (wide_slots, down_slots, in_sem, out_sem) = refs[3:19], refs[19:22], refs[22:]
    wide = landed(LAST, lands[0:4], outs[:2]) + landed(LAST + 1, lands[4:8], outs[:2])
    down = landed(LAST, lands[8:12], outs[2:]) + landed(LAST + 1, lands[12:16], outs[2:])
    through(wide, wide_slots, in_sem, out_sem)
    through(down, down_slots, in_sem, out_sem)


def in_place(pairs, sem):
    copies = [pltpu.make_async_copy(src, dst, sem.at[i]) for i, (src, dst) in enumerate(pairs)]
    for copy in copies:
        copy.start()
    for copy in copies:
        copy.wait()


def finish_wide(*refs):
    through(landed(LAST + 2, refs[2:6], refs[6:8]), *refs[8:])


def finish_deep(*refs):
    in_place(landed(LAST + 2, refs[1:5], refs[5:6], 0, pl.ds(0, 128)), refs[6])


def finish_own(*refs):
    in_place(landed(LAST + 2, refs[1:3], refs[3:4], 0, pl.ds(128, 128)), refs[4])


def finish_tail(*refs):
    in_place(landed(LAST + 2, refs[1:3], refs[3:4], 2, pl.ds(128, 128)), refs[4])


def solution(mesh):
    whole = [(2, 1024, 4096), (2, 1024, 4096), (2, 4096, 1024)]
    block = [(2, 64, 4096), (2, 64, 4096), (2, 256, 1024)]

    def shapes(dims, dtype):
        return [jax.ShapeDtypeStruct(s, dtype) for s in dims]

    def pair(lead, dtype):
        return [pltpu.VMEM((*lead, 2, 2, 64, 4096), dtype), pltpu.VMEM((*lead, 2, 256, 1024), dtype)]

    dma = pltpu.SemaphoreType.DMA
    anywhere = pl.BlockSpec(memory_space=pl.ANY)
    hbm = pl.BlockSpec(memory_space=pltpu.HBM)
    vmem = pl.BlockSpec(memory_space=pltpu.VMEM)
    mib = 1024 * 1024

    def local(body, outs, ins, scratch, moved, limit, aliases=None, specs=None):
        return call_local(body, outs, ins, scratch, moved, limit, aliases, specs)

    def call_local(body, outs, ins, scratch, moved, limit, aliases, specs):
        return pl.pallas_call(
            body,
            out_shape=outs,
            in_specs=specs or [hbm] * len(ins),
            out_specs=[hbm] * len(outs),
            scratch_shapes=scratch,
            input_output_aliases=aliases or {},
            cost_estimate=pl.CostEstimate(flops=int(moved * 40), bytes_accessed=int(moved), transcendentals=0),
            compiler_params=pltpu.CompilerParams(vmem_limit_bytes=limit * mib),
        )(*ins)

    def permute(array, pairs):
        return lax.ppermute(array, "dp", pairs)

    def at(q, c):
        return device_at(q % CHIPS, c)

    clockwise = [(at(q, c), at(q + 1, c)) for q in range(CHIPS) for c in range(2)]
    ways = [clockwise, [(b, a) for a, b in clockwise]]
    across = [(i, i ^ 1) for i in range(16)]

    def step(*arrays):
        m, v = arrays[6:9], arrays[9:12]
        out = pl.pallas_call(
            kernel,
            out_shape=[
                *shapes(whole + block, BF16),
                jax.ShapeDtypeStruct((8, 128), F32),
                *shapes([(2, 64, 4096)] * 2 + [(256, 1024)] * 2, BF16),
            ],
            in_specs=[hbm] * 12,
            out_specs=[hbm] * 6 + [vmem] + [hbm] * 4,
            scratch_shapes=[
                *pair((8,), BF16),
                *pair((3,), BF16),
                *pair((2,), BF16),
                *pair((), BF16),
                *pair((), F32),
                *pair((), F32),
                pltpu.VMEM((16, 1024), F32),
                pltpu.VMEM((16, 1, 128), F32),
                dma((2,)), dma((8, 2)), dma((2,)), dma((3, 12)), dma((2, 2)), dma((3, 2)),
                dma((2,)), dma((2,)), dma((2,)), dma((1,)), dma((1,)), dma((2,)), dma((2,)),
            ],
            compiler_params=pltpu.CompilerParams(collective_id=0, has_side_effects=True, vmem_limit_bytes=66 * 1000 * 1000),
            name="step",
        )(*arrays)
        (xg, xu, xd), sums, factor, (e0, e1, f0, f1) = out[:3], out[3:6], out[6], out[7:]
        slots = [dma((16,)), dma((16,))]

        def hop_on(arrays):
            return [permute(e, ways[d]) for d, e in enumerate(arrays)]

        def cross(arrays):
            return [permute(e, across) for e in arrays]

        wide5, deep5 = [e0, e1], [f0, f1]
        wide6, deep6 = hop_on(wide5), hop_on(deep5)
        their_wide5, their_deep5 = cross(wide5), cross(deep5)
        new_g, new_u = local(
            copy_wide, shapes(whole[:2], BF16), (xg, xu), [pltpu.VMEM((16, 128, 4096), BF16), *slots], 40 * mib, 50
        )
        wide7, their_wide6 = hop_on(wide6), cross(wide6)
        new_d, *state = local(
            copy_down,
            shapes(whole[2:], BF16) + shapes(block * 2, F32),
            (factor, xd, *sums, *m, *v),
            [
                pltpu.VMEM((16, 512, 1024), BF16), *pair((), BF16), *pair((), F32), *pair((), F32),
                *slots, dma((3, 6)), dma((2, 6)),
            ],
            48 * mib,
            50,
            specs=[vmem] + [hbm] * 10,
        )
        deep7, their_deep6 = hop_on([e[:128] for e in deep6]), cross(deep6)
        tail7 = hop_on([e[128:] for e in deep6])
        news = local(
            settle,
            shapes(whole, BF16),
            (new_g, new_u, new_d, *wide5, *their_wide5, *wide6, *their_wide6, *deep5, *their_deep5, *deep6, *their_deep6),
            [pltpu.VMEM((16, 64, 4096), BF16), pltpu.VMEM((16, 256, 1024), BF16), *slots],
            24 * mib,
            24,
            {0: 0, 1: 1, 2: 2},
            [hbm] * 3 + [anywhere] * 16,
        )
        their_wide7 = cross(wide7)
        new_g, new_u = local(
            finish_wide, shapes(whole[:2], BF16), (*news[:2], *wide7, *their_wide7),
            [pltpu.VMEM((16, 64, 4096), BF16), *slots],
            8 * mib, 24, {0: 0, 1: 1}, [hbm] * 2 + [anywhere] * 4,
        )
        their_deep7 = cross(deep7)
        their_tail7 = cross(tail7)
        (new_d,) = local(
            finish_deep, shapes(whole[2:], BF16), (news[2], *deep7, *their_deep7), [dma((4,))],
            2 * mib, 24, {0: 0}, [hbm] + [anywhere] * 4,
        )
        for body, lands in ((finish_own, tail7), (finish_tail, their_tail7)):
            (new_d,) = local(
                body, shapes(whole[2:], BF16), (new_d, *lands), [dma((2,))], mib, 24, {0: 0}, [hbm] + [anywhere] * 2
            )
        return (new_g, new_u, new_d, *state)

    all_of, cut = P(None, None, None), P(None, "dp", None)
    return jax.shard_map(
        step,
        mesh=mesh,
        in_specs=(P(("rep", "dp"), None, None, None),) * 3 + (all_of,) * 3 + (cut,) * 6,
        out_specs=(P("rep", None, None),) * 3 + (P("rep", "dp", None),) * 6,
        check_vma=False,
    )
```
